512 devices in a mesh: grp: 8 (over z), dev: 64 (over x, y, core).
Axes of the slice: x: 4, y: 8, z: 8, core: 2. Of those that a mesh axis runs over, the one named last changes fastest.
Arguments:
- points: float32 [524288, 768], P(('grp', 'dev')), may hold values from -12 to 12
- assignment: int32 [524288], P(('grp', 'dev')), may hold values from 0 to 16383, as said below
Outputs:
- centroids: float32 [16384, 768], P('dev')
- spread: float32 [16384], P('dev')
The draws below stay inside these ranges and needn't reach their ends.
Inputs may be any that keep to these rules, and one draw needn't show every extreme that they name: `assignment`: the owner of cluster c is c // 256. Among the 1024 points of one device (aligned blocks of 1024), at most 32 belong to clusters of one owner; some owner receives exactly 32 from every device's block.
All inputs are finite; a program needn't handle non-finite values.
Results may differ from the reference program's by a relative error of at most 0.000071.
Values sent between devices are 32-bit elements; how exact they have to be, the bound alone decides.
No kernel may reach another device: no remote copies, remote signals or barrier semaphores. Data moves between devices by JAX's collectives and lax.ppermute only.
A program may use at most 64 MiB of HBM per device.

```python
import jax
import jax.numpy as jnp
from jax import lax

D = 768
CL_OWN = 256
TOK_DEV = 1024
CLUSTERS = 16384
CAP = 32
POINTS = 524288


def draw_assignment(key, part):
    blocks = POINTS // TOK_DEV
    owners = CLUSTERS // CL_OWN
    total_slots = owners * CAP
    key_hot, key_score, key_order, key_within = jax.random.split(key, 4)
    hottest = jax.random.randint(key_hot, (), 0, owners)
    scores = jax.random.randint(key_score, (blocks, total_slots), 0, 1 << 16)
    slot_owner = jnp.arange(total_slots, dtype=jnp.int32) // CAP
    scores = jnp.where(slot_owner[None, :] == hottest, scores + (1 << 17), scores)
    distinct = scores * total_slots + jnp.arange(total_slots, dtype=jnp.int32)[None, :]
    _, chosen = lax.top_k(distinct, TOK_DEV)
    shuffle = jax.random.randint(key_order, (blocks, TOK_DEV), 0, 1 << 18)
    shuffle = shuffle * TOK_DEV + jnp.arange(TOK_DEV, dtype=jnp.int32)[None, :]
    order = jnp.argsort(shuffle, axis=1)
    picked = jnp.take_along_axis(chosen.astype(jnp.int32), order, axis=1)
    owner = picked // CAP
    within = jax.random.randint(key_within, (blocks, TOK_DEV), 0, CL_OWN)
    return (owner * CL_OWN + within).reshape(-1).astype(jnp.int32)


def block_levels(stream_key, dims, shards, smallest, largest):
    gain, own = 1.0, jax.random.fold_in(stream_key, 6)
    for dim, parts in shards:
        steps = jnp.exp(jax.random.uniform(jax.random.fold_in(own, dim), (parts,), jnp.float32, smallest / len(shards), largest / len(shards)))
        gain = gain * jnp.repeat(steps, dims[dim] // parts).reshape([-1 if axis == dim else 1 for axis in range(len(dims))])
    return gain


def bell_draw(stream_key, extent, width, limit, shards=(), held_as=jnp.bfloat16):
    drawn = width * jax.random.normal(stream_key, extent, jnp.float32)
    if shards:
        drawn = drawn * block_levels(stream_key, extent, shards, -0.22, 0.18)
    return jnp.clip(drawn, -limit, limit).astype(held_as)


def setup_inputs(seed: int = 0) -> dict:
    key_of = jax.random.split(jax.random.key(seed), 3)
    points = bell_draw(key_of[0], (POINTS, D), 2.0, 12.0, ((0, 512),), jnp.float32)
    assignment = draw_assignment(jax.random.fold_in(key_of[2], 71), 0)
    return dict(points=points, assignment=assignment)


def reference(points, assignment):
    sums = jax.ops.segment_sum(points, assignment, num_segments=CLUSTERS)
    counts = jax.ops.segment_sum(jnp.ones(assignment.shape, jnp.float32), assignment, num_segments=CLUSTERS)
    squares = jax.ops.segment_sum(jnp.sum(points * points, axis=1), assignment, num_segments=CLUSTERS)
    denom = jnp.maximum(counts, 1.0)
    centroids = sums / denom[:, None]
    spread = (squares - jnp.sum(sums * sums, axis=1) / denom) / (denom * D)
    return centroids, spread
```

```python
import jax
import jax.numpy as jnp
from jax import lax
from jax.experimental import pallas as pl
from jax.experimental.pallas import tpu as pltpu
from jax.sharding import Mesh
from jax.sharding import PartitionSpec as P

CL_OWN = 256
OWNERS = 64
LANES = 128
CAP = 32
MERGE = 32
PAIR = OWNERS // MERGE
SLOTS = PAIR * CAP
PARTS = 8
ROWS = CL_OWN // PARTS
SPREAD = PAIR * PARTS


def split3(value):
    first = value.astype(jnp.bfloat16)
    rest = value - first.astype(jnp.float32)
    second = rest.astype(jnp.bfloat16)
    third = (rest - second.astype(jnp.float32)).astype(jnp.bfloat16)
    return first, second, third


def pack_kernel(row_ref, left_ref, right_ref, aux_ref, out_ref):
    step = pl.program_id(0)
    last = pl.num_programs(0) - 1
    group = 2 * SLOTS

    @pl.when(step < last)
    def _():
        flat = out_ref.reshape(MERGE * group, LANES)

        def clear(g, carry):
            start = pl.multiple_of(g * group, 8)
            flat[pl.ds(start, group), :] = jnp.zeros((group, LANES), jnp.float32)
            return carry

        lax.fori_loop(0, MERGE, clear, 0)

        def place(i, carry):
            for r in range(8):
                at = row_ref[i * 8 + r]
                flat[pl.ds(at, 1), :] = left_ref[pl.ds(i * 8 + r, 1), :]
                flat[pl.ds(at + SLOTS, 1), :] = right_ref[pl.ds(i * 8 + r, 1), :]
            return carry

        lax.fori_loop(0, left_ref.shape[0] // 8, place, 0)

    @pl.when(step == last)
    def _():
        out_ref[:, :8, :] = aux_ref[...]


def pack(row, points, aux):
    rows, width = points.shape
    blocks = width // LANES
    steps = blocks // 2
    return pl.pallas_call(
        pack_kernel,
        grid=(steps + 1,),
        out_shape=jax.ShapeDtypeStruct((MERGE, blocks * SLOTS + 8, LANES), jnp.float32),
        in_specs=[
            pl.BlockSpec(memory_space=pltpu.SMEM),
            pl.BlockSpec((rows, LANES), lambda k: (0, 2 * jnp.minimum(k, steps - 1))),
            pl.BlockSpec((rows, LANES), lambda k: (0, 2 * jnp.minimum(k, steps - 1) + 1)),
            pl.BlockSpec(aux.shape, lambda k: (0, 0, 0)),
        ],
        out_specs=pl.BlockSpec((MERGE, 2 * SLOTS, LANES), lambda k: (0, k, 0)),
        compiler_params=pltpu.CompilerParams(vmem_limit_bytes=40 * 1024 * 1024),
        name="pack",
    )(row, points, points, aux)


def target_of(pair, part):
    return (2 * pair + part % 2) * 4 + part // 2


def merge_kernel(tags_ref, squares_ref, arrived_ref, out_ref, hot_ref):
    step = pl.program_id(0)
    tail = out_ref.shape[1] - 8

    @pl.when(step == 0)
    def _():
        cluster = lax.broadcasted_iota(jnp.int32, (CL_OWN, MERGE * CAP), 0) + 1
        for a in range(PAIR):
            tag = tags_ref[pl.ds(a, 1), :].astype(jnp.int32)
            hot = (cluster == tag).astype(jnp.float32).astype(jnp.bfloat16)
            hot_ref[a] = hot
            one, two, three = split3(squares_ref[pl.ds(a, 1), :])
            row = lax.broadcasted_iota(jnp.int32, (8, MERGE * CAP), 0)
            values = jnp.where(row == 0, 1.0, 0.0)
            values = jnp.where(row == 1, one.astype(jnp.float32), values)
            values = jnp.where(row == 2, two.astype(jnp.float32), values)
            values = jnp.where(row == 3, three.astype(jnp.float32), values)
            small = lax.dot_general(
                values.astype(jnp.bfloat16),
                hot,
                (((1,), (1,)), ((), ())),
                preferred_element_type=jnp.float32,
            )
            for part in range(PARTS):
                low = part * ROWS // LANES * LANES
                out_ref[target_of(a, part), tail:, :] = small[:, low : low + LANES]

    for a in range(PAIR):
        data = jnp.concatenate(
            [
                arrived_ref[:, j * SLOTS + a * CAP : j * SLOTS + (a + 1) * CAP, :].reshape(
                    MERGE * CAP, LANES
                )
                for j in range(2)
            ],
            axis=1,
        )
        hot = hot_ref[a]
        total = sum(
            jnp.dot(hot, term, preferred_element_type=jnp.float32)
            for term in reversed(split3(data))
        )
        for part in range(PARTS):
            for j in range(2):
                start = pl.multiple_of((2 * step + j) * ROWS, 8)
                out_ref[target_of(a, part), pl.ds(start, ROWS), :] = total[
                    part * ROWS : (part + 1) * ROWS, j * LANES : (j + 1) * LANES
                ]


def merge(tags, squares, arrived):
    blocks = (arrived.shape[1] - 8) // SLOTS
    shape = (SPREAD, blocks * ROWS + 8, LANES)
    return pl.pallas_call(
        merge_kernel,
        grid=(blocks // 2,),
        out_shape=jax.ShapeDtypeStruct(shape, jnp.float32),
        in_specs=[
            pl.BlockSpec(tags.shape, lambda k: (0, 0)),
            pl.BlockSpec(squares.shape, lambda k: (0, 0)),
            pl.BlockSpec((MERGE, 2 * SLOTS, LANES), lambda k: (0, k, 0)),
        ],
        out_specs=pl.BlockSpec(shape, lambda k: (0, 0, 0)),
        scratch_shapes=[pltpu.VMEM((PAIR, CL_OWN, MERGE * CAP), jnp.bfloat16)],
        compiler_params=pltpu.CompilerParams(vmem_limit_bytes=40 * 1024 * 1024),
        name="merge",
    )(tags, squares, arrived)


def finish_kernel(offset_ref, arrived_ref, out_ref):
    tail = out_ref.shape[0] - 8
    blocks = tail // ROWS
    total = arrived_ref[0]
    for k in range(1, SPREAD):
        total = total + arrived_ref[k]
    row = lax.broadcasted_iota(jnp.int32, (ROWS, LANES), 0)
    lane = lax.broadcasted_iota(jnp.int32, (ROWS, LANES), 1)
    mine = lane == row + offset_ref[0]
    squares = total[tail + 1 : tail + 2] + total[tail + 2 : tail + 3] + total[tail + 3 : tail + 4]
    counts = jnp.sum(jnp.where(mine, total[tail : tail + 1], 0.0), axis=1, keepdims=True)
    squares = jnp.sum(jnp.where(mine, squares, 0.0), axis=1, keepdims=True)
    denom = jnp.maximum(counts, 1.0)
    norm = jnp.zeros((ROWS, LANES), jnp.float32)
    for j in range(blocks):
        sums = total[j * ROWS : (j + 1) * ROWS]
        norm = norm + sums * sums
        out_ref[j * ROWS : (j + 1) * ROWS, :] = sums / denom
    norm = jnp.sum(norm, axis=1, keepdims=True)
    spread = (squares - norm / denom) / (denom * (blocks * LANES))
    flat = jnp.sum(jnp.where(lane == row, spread, 0.0), axis=0, keepdims=True)
    out_ref[tail:, :] = jnp.broadcast_to(flat, (8, LANES))


def finish(offset, arrived):
    return pl.pallas_call(
        finish_kernel,
        out_shape=jax.ShapeDtypeStruct(arrived.shape[1:], jnp.float32),
        in_specs=[
            pl.BlockSpec(memory_space=pltpu.SMEM),
            pl.BlockSpec(memory_space=pltpu.VMEM),
        ],
        out_specs=pl.BlockSpec(memory_space=pltpu.VMEM),
        name="finish",
    )(offset, arrived)


def body(points, assignment):
    rows, width = points.shape
    blocks = width // LANES
    owner = assignment >> 8
    label = assignment & (CL_OWN - 1)
    slot = ((owner >> 4) * 8 + (owner & 7)) * 2 + ((owner >> 3) & 1)
    matches = slot[:, None] == jnp.arange(OWNERS, dtype=jnp.int32)[None, :]
    matches = matches.astype(jnp.float32)
    earlier = (jnp.arange(rows)[:, None] > jnp.arange(rows)[None, :]).astype(jnp.float32)
    before = jnp.dot(earlier, matches, preferred_element_type=jnp.float32)
    position = jnp.sum(before * matches, axis=1).astype(jnp.int32)
    row = (slot >> 1) * (2 * SLOTS) + (slot & 1) * CAP + position
    at = (position[:, None] == jnp.arange(CAP, dtype=jnp.int32)[None, :]).astype(jnp.float32)
    norms = jnp.sum(points * points, axis=1)
    values = jnp.concatenate(
        [at * (label + 1).astype(jnp.float32)[:, None], at * norms[:, None]], axis=1
    )
    placed = lax.dot_general(
        matches,
        values,
        (((0,), (0,)), ((), ())),
        precision=lax.Precision.HIGHEST,
        preferred_element_type=jnp.float32,
    )
    aux = placed.reshape(MERGE, PAIR, 2, CAP).transpose(0, 2, 1, 3).reshape(MERGE, 2, SLOTS)
    aux = jnp.pad(aux, ((0, 0), (0, 6), (0, LANES - SLOTS)))

    outgoing = pack(row, points, aux)
    arrived = lax.all_to_all(
        outgoing, ("x", "zb", "yb", "c"), split_axis=0, concat_axis=0, tiled=True
    )
    info = arrived[:, blocks * SLOTS : blocks * SLOTS + 2, :SLOTS]
    info = info.reshape(MERGE, 2, PAIR, CAP).transpose(1, 2, 0, 3).reshape(2, PAIR, MERGE * CAP)

    partial = merge(info[0], info[1], arrived)
    arrived = lax.all_to_all(partial, ("yp", "zp"), split_axis=0, concat_axis=0, tiled=True)

    part = 2 * lax.axis_index("zp") + lax.axis_index("yp") % 2
    offset = (part * ROWS % LANES).astype(jnp.int32).reshape(1)
    done = finish(offset, arrived)
    moves = []
    for zb in range(2):
        for yp in range(4):
            here = zb * 4 + yp
            moves.append((here, here if yp % 2 == zb else (zb ^ 1) * 4 + (yp ^ 1)))
    done = lax.ppermute(done, ("zb", "yp"), moves)
    whole = lax.all_gather(done, ("zp", "zb"), axis=0, tiled=False)
    centre = whole[:, : blocks * ROWS].reshape(PARTS, blocks, ROWS, LANES)
    centre = centre.transpose(0, 2, 1, 3).reshape(CL_OWN, width)
    spread = whole[:, blocks * ROWS, :ROWS].reshape(CL_OWN)
    return centre, spread


def solution(mesh):
    fine = Mesh(
        mesh.devices.reshape(4, 2, 4, 4, 2, 2), ("zp", "zb", "x", "yp", "yb", "c")
    )
    every = ("zp", "zb", "x", "yp", "yb", "c")
    owners = ("x", "yp", "yb", "c")
    return jax.shard_map(
        body,
        mesh=fine,
        in_specs=(P(every, None), P(every)),
        out_specs=(P(owners, None), P(owners)),
        check_vma=False,
    )
```

```python
import jax
import jax.numpy as jnp
from jax import lax
from jax.experimental import pallas as pl
from jax.experimental.pallas import tpu as pltpu
from jax.sharding import Mesh
from jax.sharding import PartitionSpec as P

CL_OWN = 256
OWNERS = 64
LANES = 128
CAP = 32
MERGE = 32
PAIR = OWNERS // MERGE
SLOTS = PAIR * CAP
PARTS = 8
ROWS = CL_OWN // PARTS
SIDE = 4
KEYS = MERGE * CAP
GATHER = LANES // CAP
TAIL = 8


def split3(value):
    first = value.astype(jnp.bfloat16)
    rest = value - first.astype(jnp.float32)
    second = rest.astype(jnp.bfloat16)
    third = (rest - second.astype(jnp.float32)).astype(jnp.bfloat16)
    return first, second, third


def whole(space=pltpu.VMEM):
    return pl.BlockSpec(memory_space=space)


def params():
    return pltpu.CompilerParams(vmem_limit_bytes=48 * 1024 * 1024)


def pack_kernel(row_ref, *refs):
    *block_refs, aux_ref, out_ref = refs
    blocks = len(block_refs)
    stride = blocks * SLOTS + TAIL
    flat = out_ref.reshape(MERGE * stride, LANES)

    def clear(g, carry):
        start = pl.multiple_of(g * stride, 8)
        flat[pl.ds(start, stride - TAIL), :] = jnp.zeros((stride - TAIL, LANES), jnp.float32)
        flat[pl.ds(start + stride - TAIL, TAIL), :] = aux_ref[g]
        return carry

    lax.fori_loop(0, MERGE, clear, 0)

    def place(i, carry):
        for r in range(8):
            at = row_ref[i * 8 + r]
            for j, ref in enumerate(block_refs):
                flat[pl.ds(at + j * SLOTS, 1), :] = ref[pl.ds(i * 8 + r, 1), :]
        return carry

    lax.fori_loop(0, block_refs[0].shape[0] // 8, place, 0)


def pack(row, points, aux, first, blocks):
    rows = points.shape[0]

    def column(j):
        return pl.BlockSpec((rows, LANES), lambda i: (0, j))

    shape = (MERGE, blocks * SLOTS + TAIL, LANES)
    return pl.pallas_call(
        pack_kernel,
        grid=(1,),
        out_shape=jax.ShapeDtypeStruct(shape, jnp.float32),
        in_specs=[
            pl.BlockSpec(memory_space=pltpu.SMEM),
            *[column(first + j) for j in range(blocks)],
            pl.BlockSpec(aux.shape, lambda i: (0, 0, 0)),
        ],
        out_specs=pl.BlockSpec(shape, lambda i: (0, 0, 0)),
        compiler_params=params(),
        name="pack",
    )(row, *[points] * blocks, aux)


def lane_rows(arrived_ref):
    tail = arrived_ref.shape[1] - TAIL
    tiles = []
    for k in range(MERGE // GATHER):
        tile = arrived_ref[k * GATHER, tail:, :]
        for s in range(1, GATHER):
            tile = tile + arrived_ref[k * GATHER + s, tail:, :]
        tiles.append(tile)
    return jnp.concatenate(tiles, axis=1)


def one_hot(tags):
    cluster = lax.broadcasted_iota(jnp.int32, (CL_OWN, KEYS), 0) + 1
    return (cluster == tags.astype(jnp.int32)).astype(jnp.float32).astype(jnp.bfloat16)


def owner_sums(hot, arrived_ref, a):
    blocks = (arrived_ref.shape[1] - TAIL) // SLOTS
    terms = []
    for j in range(blocks):
        low = j * SLOTS + a * CAP
        terms.append(split3(arrived_ref[:, low : low + CAP, :].reshape(KEYS, LANES)))
    columns = jnp.concatenate([t[k] for k in range(3) for t in terms], axis=1)
    total = jnp.dot(hot, columns, preferred_element_type=jnp.float32)
    wide = blocks * LANES
    return total[:, 2 * wide :] + total[:, wide : 2 * wide] + total[:, :wide]


def row_sums(hot, rows):
    return lax.dot_general(
        rows.astype(jnp.bfloat16), hot, (((1,), (1,)), ((), ())), preferred_element_type=jnp.float32
    )


def merge_a_kernel(side_ref, arrived_ref, tags_ref, *refs):
    *out_refs, sums_ref, small_ref = refs
    blocks = (arrived_ref.shape[1] - TAIL) // SLOTS
    tags = lane_rows(arrived_ref)
    tags_ref[...] = tags
    for a in range(PAIR):
        hot = one_hot(tags[a : a + 1])
        row = lax.broadcasted_iota(jnp.int32, (TAIL, KEYS), 0)
        small_ref[a] = row_sums(hot, jnp.where(row == 0, 1.0, 0.0))
        sums_ref[a] = owner_sums(hot, arrived_ref, a)
    for k in range(SIDE):
        there = (side_ref[0] + k) & (SIDE - 1)
        a = there >> 1
        odd = there & 1
        for zp in range(SIDE):
            low = pl.multiple_of((2 * zp + odd) * ROWS, ROWS)
            sums = sums_ref[a, pl.ds(low, ROWS), :]
            for j in range(blocks):
                out_refs[k][zp, j * ROWS : (j + 1) * ROWS, :] = sums[
                    :, j * LANES : (j + 1) * LANES
                ]
            half = 2 * zp * ROWS // LANES * LANES
            out_refs[k][zp, blocks * ROWS :, :] = small_ref[a, :, half : half + LANES]


def merge_a(side, arrived):
    blocks = (arrived.shape[1] - TAIL) // SLOTS
    part = jax.ShapeDtypeStruct((SIDE, blocks * ROWS + TAIL, LANES), jnp.float32)
    return pl.pallas_call(
        merge_a_kernel,
        out_shape=[jax.ShapeDtypeStruct((TAIL, KEYS), jnp.float32), *[part] * SIDE],
        in_specs=[whole(pltpu.SMEM), whole()],
        out_specs=[whole()] * (SIDE + 1),
        scratch_shapes=[
            pltpu.VMEM((PAIR, CL_OWN, blocks * LANES), jnp.float32),
            pltpu.VMEM((PAIR, TAIL, CL_OWN), jnp.float32),
        ],
        compiler_params=params(),
        name="merge_a",
    )(side, arrived)


def merge_b_kernel(tags_ref, arrived_ref, after_ref, out_ref):
    blocks = (arrived_ref.shape[1] - TAIL) // SLOTS
    norms = lane_rows(arrived_ref)
    for a in range(PAIR):
        hot = one_hot(tags_ref[a : a + 1, :])
        one, two, three = split3(norms[a : a + 1])
        row = lax.broadcasted_iota(jnp.int32, (TAIL, KEYS), 0)
        values = jnp.where(row == 0, one.astype(jnp.float32), 0.0)
        values = jnp.where(row == 1, two.astype(jnp.float32), values)
        values = jnp.where(row == 2, three.astype(jnp.float32), values)
        small = row_sums(hot, values)
        total = owner_sums(hot, arrived_ref, a)
        for part in range(PARTS):
            target = (2 * a + part % 2) * SIDE + part // 2
            for j in range(blocks):
                out_ref[target, j * ROWS : (j + 1) * ROWS, :] = total[
                    part * ROWS : (part + 1) * ROWS, j * LANES : (j + 1) * LANES
                ]
            half = part * ROWS // LANES * LANES
            out_ref[target, blocks * ROWS :, :] = small[:, half : half + LANES]


def merge_b(tags, arrived, after):
    blocks = (arrived.shape[1] - TAIL) // SLOTS
    shape = (SIDE * SIDE, blocks * ROWS + TAIL, LANES)
    return pl.pallas_call(
        merge_b_kernel,
        out_shape=jax.ShapeDtypeStruct(shape, jnp.float32),
        in_specs=[whole(), whole(), whole(pl.ANY)],
        out_specs=whole(),
        compiler_params=params(),
        name="merge_b",
    )(tags, arrived, after)


def add_kernel(side_ref, own_ref, *refs):
    *in_refs, sums_ref = refs[: SIDE - 1] + refs[-1:]
    out_refs = refs[SIDE - 1 : -1]
    sums_ref[...] = own_ref[...] + in_refs[0][...] + in_refs[1][...] + in_refs[2][...]
    for k in range(SIDE):
        out_refs[k][...] = sums_ref[(side_ref[0] + k) & (SIDE - 1)]


def add(side, own, others):
    part = jax.ShapeDtypeStruct(own.shape[1:], jnp.float32)
    return pl.pallas_call(
        add_kernel,
        out_shape=[part] * SIDE,
        in_specs=[whole(pltpu.SMEM)] + [whole()] * SIDE,
        out_specs=[whole()] * SIDE,
        scratch_shapes=[pltpu.VMEM(own.shape, jnp.float32)],
        compiler_params=params(),
        name="add",
    )(side, own, *others)


def column_of(row, offset):
    at = lax.broadcasted_iota(jnp.int32, (ROWS, LANES), 0) + offset
    lane = lax.broadcasted_iota(jnp.int32, (ROWS, LANES), 1)
    return jnp.sum(jnp.where(lane == at, row, 0.0), axis=1, keepdims=True)


def finish_a_kernel(offset_ref, own_ref, one_ref, two_ref, three_ref, out_ref, denom_ref, norm_ref):
    total = own_ref[...] + one_ref[...] + two_ref[...] + three_ref[...]
    tail = total.shape[0] - TAIL
    denom = jnp.maximum(column_of(total[tail : tail + 1], offset_ref[0]), 1.0)
    norm = jnp.zeros((ROWS, LANES), jnp.float32)
    for low in range(0, tail, ROWS):
        sums = total[low : low + ROWS]
        norm = norm + sums * sums
        out_ref[low : low + ROWS, :] = sums / denom
    denom_ref[...] = jnp.broadcast_to(denom, (ROWS, LANES))
    norm_ref[...] = norm


def finish_a(offset, own, others):
    tile = jax.ShapeDtypeStruct((ROWS, LANES), jnp.float32)
    return pl.pallas_call(
        finish_a_kernel,
        out_shape=[
            jax.ShapeDtypeStruct((own.shape[0] - TAIL, LANES), jnp.float32),
            tile,
            tile,
        ],
        in_specs=[whole(pltpu.SMEM)] + [whole()] * SIDE,
        out_specs=[whole()] * 3,
        compiler_params=params(),
        name="finish_a",
    )(offset, own, *others)


def finish_b_kernel(width, offset_ref, arrived_ref, denom_ref, norm_ref, after_ref, out_ref):
    total = arrived_ref[0]
    for k in range(1, SIDE * SIDE):
        total = total + arrived_ref[k]
    tail = total.shape[0] - TAIL
    squares = total[tail : tail + 1] + total[tail + 1 : tail + 2] + total[tail + 2 : tail + 3]
    squares = column_of(squares, offset_ref[0])
    denom = denom_ref[:, :1]
    norm = norm_ref[...]
    for low in range(0, tail, ROWS):
        sums = total[low : low + ROWS]
        norm = norm + sums * sums
        out_ref[low : low + ROWS, :] = sums / denom
    norm = jnp.sum(norm, axis=1, keepdims=True)
    spread = (squares - norm / denom) / (denom * width)
    row = lax.broadcasted_iota(jnp.int32, (ROWS, LANES), 0)
    lane = lax.broadcasted_iota(jnp.int32, (ROWS, LANES), 1)
    flat = jnp.sum(jnp.where(lane == row, spread, 0.0), axis=0, keepdims=True)
    out_ref[tail:, :] = jnp.broadcast_to(flat, (TAIL, LANES))


def finish_b(width, offset, arrived, denom, norm, after):
    return pl.pallas_call(
        lambda *refs: finish_b_kernel(width, *refs),
        out_shape=jax.ShapeDtypeStruct(arrived.shape[1:], jnp.float32),
        in_specs=[whole(pltpu.SMEM)] + [whole()] * 3 + [whole(pl.ANY)],
        out_specs=whole(),
        compiler_params=params(),
        name="finish_b",
    )(offset, arrived, denom, norm, after)


def lay_kernel(a_ref, b_ref, out_ref):
    blocks = out_ref.shape[1] // LANES
    left = a_ref.shape[1] // ROWS
    for part in range(PARTS):
        for j in range(blocks):
            ref, at = (a_ref, j) if j < left else (b_ref, j - left)
            out_ref[part * ROWS : (part + 1) * ROWS, j * LANES : (j + 1) * LANES] = ref[
                part, at * ROWS : (at + 1) * ROWS, :
            ]


def lay(a, b, width):
    return pl.pallas_call(
        lay_kernel,
        out_shape=jax.ShapeDtypeStruct((CL_OWN, width), jnp.float32),
        in_specs=[whole(), whole()],
        out_specs=whole(),
        compiler_params=params(),
        name="lay",
    )(a, b)


def shifted(parts, axis):
    return [
        lax.ppermute(part, axis, [(j, (j + k) % SIDE) for j in range(SIDE)])
        for k, part in enumerate(parts, 1)
    ]


def to_owner(value):
    moves = []
    for zb in range(2):
        for yp in range(SIDE):
            here = zb * SIDE + yp
            moves.append((here, here if yp % 2 == zb else (zb ^ 1) * SIDE + (yp ^ 1)))
    value = lax.ppermute(value, ("zb", "yp"), moves)
    return lax.all_gather(value, ("zp", "zb"), axis=0, tiled=False)


def meet(value):
    return lax.all_to_all(value, ("x", "zb", "yb", "c"), split_axis=0, concat_axis=0, tiled=True)


def body(points, assignment):
    rows, width = points.shape
    blocks = width // LANES
    left = blocks // 2
    owner = assignment >> 8
    label = assignment & (CL_OWN - 1)
    slot = ((owner >> 4) * 8 + (owner & 7)) * 2 + ((owner >> 3) & 1)
    matches = slot[:, None] == jnp.arange(OWNERS, dtype=jnp.int32)[None, :]
    matches = matches.astype(jnp.float32)
    earlier = (jnp.arange(rows)[:, None] > jnp.arange(rows)[None, :]).astype(jnp.float32)
    before = jnp.dot(earlier, matches, preferred_element_type=jnp.float32)
    position = jnp.sum(before * matches, axis=1).astype(jnp.int32)
    inside = (slot & 1) * CAP + position
    row_a = (slot >> 1) * (left * SLOTS + TAIL) + inside
    row_b = (slot >> 1) * ((blocks - left) * SLOTS + TAIL) + inside
    place = position[:, None] == jnp.arange(CAP, dtype=jnp.int32)[None, :]
    group = (lax.axis_index("yb") * 2 + lax.axis_index("c")) % GATHER
    lanes = jnp.arange(LANES, dtype=jnp.int32)[None, None, :] // CAP == group

    def tails(value, precision):
        at = jnp.where(place, value[:, None], 0.0)
        placed = lax.dot_general(
            matches,
            at,
            (((0,), (0,)), ((), ())),
            precision=precision,
            preferred_element_type=jnp.float32,
        )
        placed = jnp.tile(placed.reshape(MERGE, PAIR, CAP), (1, 1, GATHER))
        return jnp.pad(jnp.where(lanes, placed, 0.0), ((0, 0), (0, TAIL - PAIR), (0, 0)))

    yp = lax.axis_index("yp")
    zp = lax.axis_index("zp")
    offset = ((2 * zp + (yp & 1)) * ROWS % LANES).reshape(1)

    tags = tails((label + 1).astype(jnp.float32), lax.Precision.DEFAULT)
    packed = pack(row_a, points, tags, 0, left)
    met_a = meet(packed)
    later, _ = lax.optimization_barrier((points, packed))
    norms = tails(jnp.sum(later * later, axis=1), lax.Precision.HIGHEST)
    met_b = meet(pack(row_b, points, norms, left, blocks - left))

    tags, own, *rest = merge_a(yp.reshape(1), met_a)
    own, *rest = add(zp.reshape(1), own, shifted(rest, "yp"))
    done_a, denom, norm = finish_a(offset, own, shifted(rest, "zp"))
    all_a = to_owner(done_a)

    partial = merge_b(tags, met_b, denom)
    partial = lax.all_to_all(partial, ("yp", "zp"), split_axis=0, concat_axis=0, tiled=True)
    all_b = to_owner(finish_b(width, offset, partial, denom, norm, all_a))
    centre = lay(all_a, all_b, width)
    spread = all_b[:, -TAIL, :ROWS].reshape(CL_OWN)
    return centre, spread


def solution(mesh):
    fine = Mesh(mesh.devices.reshape(4, 2, 4, 4, 2, 2), ("zp", "zb", "x", "yp", "yb", "c"))
    every = ("zp", "zb", "x", "yp", "yb", "c")
    owners = ("x", "yp", "yb", "c")
    return jax.shard_map(
        body,
        mesh=fine,
        in_specs=(P(every, None), P(every)),
        out_specs=(P(owners, None), P(owners)),
        check_vma=False,
    )
```

```python
import jax
import jax.numpy as jnp
from jax import lax
from jax.experimental import pallas as pl
from jax.experimental.pallas import tpu as pltpu
from jax.sharding import Mesh
from jax.sharding import PartitionSpec as P

CL_OWN = 256
OWNERS = 64
LANES = 128
CAP = 32
SIDE = 4
GROUPS = OWNERS // SIDE
HALVES = 2
MERGE = GROUPS * HALVES
SLOTS = SIDE * CAP
ROWS = CL_OWN // SIDE
KEYS = MERGE * CAP
TAIL = 8


def split3(value):
    first = value.astype(jnp.bfloat16)
    rest = value - first.astype(jnp.float32)
    second = rest.astype(jnp.bfloat16)
    third = (rest - second.astype(jnp.float32)).astype(jnp.bfloat16)
    return first, second, third


def whole(space=pltpu.VMEM):
    return pl.BlockSpec(memory_space=space)


def params(mib):
    return pltpu.CompilerParams(vmem_limit_bytes=mib * 1024 * 1024)


def pack_kernel(row_ref, points_ref, tags_ref, out_ref):
    rows, width = points_ref.shape
    blocks = width // LANES // HALVES
    stride = blocks * SLOTS + TAIL
    flat = out_ref.reshape(MERGE * stride, LANES)

    def clear(g, carry):
        start = pl.multiple_of(g * stride, 8)
        flat[pl.ds(start, stride - TAIL), :] = jnp.zeros((stride - TAIL, LANES), jnp.float32)
        flat[pl.ds(start + stride - TAIL, TAIL), :] = tags_ref[g & (GROUPS - 1)]
        return carry

    lax.fori_loop(0, MERGE, clear, 0)

    def place(i, carry):
        start = pl.multiple_of(i * 8, 8)
        ats = [row_ref[i * 8 + r] for r in range(8)]
        for h in range(HALVES):
            for j in range(blocks):
                low = (h * blocks + j) * LANES
                tile = points_ref[pl.ds(start, 8), low : low + LANES]
                for r in range(8):
                    at = ats[r] + (h * GROUPS * stride + j * SLOTS)
                    flat[pl.ds(at, 1), :] = tile[r : r + 1]
        return carry

    lax.fori_loop(0, rows // 8, place, 0)


def pack(row, points, tags):
    blocks = points.shape[1] // LANES // HALVES
    return pl.pallas_call(
        pack_kernel,
        out_shape=jax.ShapeDtypeStruct((MERGE, blocks * SLOTS + TAIL, LANES), jnp.float32),
        in_specs=[whole(pltpu.SMEM), whole(), whole()],
        out_specs=whole(),
        compiler_params=params(12),
        name="pack",
    )(row, points, tags)


def merge_kernel(arrived_ref, out_ref, hot_ref, square_ref):
    blocks = (arrived_ref.shape[1] - TAIL) // SLOTS
    tail = blocks * SLOTS
    gather = LANES // CAP
    tiles = []
    for k in range(MERGE // gather):
        tile = arrived_ref[k * gather, tail:, :]
        for s in range(1, gather):
            tile = tile + arrived_ref[k * gather + s, tail:, :]
        tiles.append(tile)
    tags = jnp.concatenate(tiles, axis=1).astype(jnp.int32)
    cluster = lax.broadcasted_iota(jnp.int32, (CL_OWN, KEYS), 0) + 1
    for m in range(SIDE):
        hot = (cluster == tags[m : m + 1]).astype(jnp.float32).astype(jnp.bfloat16)
        hot_ref[m] = hot
        for j in range(blocks):
            low = j * SLOTS + m * CAP
            data = arrived_ref[:, low : low + CAP, :].reshape(KEYS, LANES)
            squares = data * data
            square_ref[...] = squares if j == 0 else square_ref[...] + squares
            terms = jnp.concatenate(split3(data), axis=1)
            total = jnp.dot(hot_ref[m], terms, preferred_element_type=jnp.float32)
            total = total[:, 2 * LANES :] + total[:, LANES : 2 * LANES] + total[:, :LANES]
            for zp in range(SIDE):
                out_ref[m * SIDE + zp, j * ROWS : (j + 1) * ROWS, :] = total[
                    zp * ROWS : (zp + 1) * ROWS
                ]
        ones = jnp.ones((TAIL, LANES), jnp.bfloat16)
        norms = sum(
            lax.dot_general(
                ones, term, (((1,), (1,)), ((), ())), preferred_element_type=jnp.float32
            )
            for term in reversed(split3(square_ref[...]))
        )
        row = lax.broadcasted_iota(jnp.int32, (TAIL, KEYS), 0)
        values = jnp.where(row == 0, 1.0, 0.0)
        for k, term in enumerate(split3(norms), 1):
            values = jnp.where(row == k, term.astype(jnp.float32), values)
        small = lax.dot_general(
            values.astype(jnp.bfloat16),
            hot_ref[m],
            (((1,), (1,)), ((), ())),
            preferred_element_type=jnp.float32,
        )
        for zp in range(SIDE):
            low = zp * ROWS // LANES * LANES
            out_ref[m * SIDE + zp, blocks * ROWS :, :] = small[:, low : low + LANES]


def merge(arrived):
    blocks = (arrived.shape[1] - TAIL) // SLOTS
    return pl.pallas_call(
        merge_kernel,
        out_shape=jax.ShapeDtypeStruct((SIDE * SIDE, blocks * ROWS + TAIL, LANES), jnp.float32),
        in_specs=[whole()],
        out_specs=whole(),
        scratch_shapes=[
            pltpu.VMEM((SIDE, CL_OWN, KEYS), jnp.bfloat16),
            pltpu.VMEM((KEYS, LANES), jnp.float32),
        ],
        compiler_params=params(16),
        name="merge",
    )(arrived)


def finish_kernel(offset_ref, arrived_ref, out_ref):
    total = arrived_ref[0]
    for k in range(1, SIDE * SIDE):
        total = total + arrived_ref[k]
    tail = total.shape[0] - TAIL
    row = lax.broadcasted_iota(jnp.int32, (ROWS, LANES), 0)
    lane = lax.broadcasted_iota(jnp.int32, (ROWS, LANES), 1)
    mine = lane == row + offset_ref[0]
    counts = jnp.sum(jnp.where(mine, total[tail : tail + 1], 0.0), axis=1, keepdims=True)
    denom = jnp.maximum(counts, 1.0)
    norm = jnp.zeros((ROWS, LANES), jnp.float32)
    for low in range(0, tail, ROWS):
        sums = total[low : low + ROWS]
        norm = norm + sums * sums
        out_ref[low : low + ROWS, :] = sums / denom
    norm = jnp.sum(norm, axis=1, keepdims=True)
    norm = jnp.sum(jnp.where(mine, norm, 0.0), axis=0, keepdims=True)
    squares = total[tail + 1 : tail + 2] + total[tail + 2 : tail + 3] + total[tail + 3 : tail + 4]
    line = lax.broadcasted_iota(jnp.int32, (TAIL, LANES), 0)
    last = jnp.where(line == 0, total[tail : tail + 1], 0.0)
    last = jnp.where(line == 1, squares, last)
    out_ref[tail:, :] = jnp.where(line == 2, norm, last)


def finish(offset, arrived):
    return pl.pallas_call(
        finish_kernel,
        out_shape=jax.ShapeDtypeStruct(arrived.shape[1:], jnp.float32),
        in_specs=[whole(pltpu.SMEM), whole()],
        out_specs=whole(),
        compiler_params=params(6),
        name="finish",
    )(offset, arrived)


def lay_kernel(all_ref, centre_ref, spread_ref):
    width = centre_ref.shape[1]
    blocks = width // LANES // HALVES
    tail = blocks * ROWS
    for zp in range(SIDE):
        for zb in range(HALVES):
            for j in range(blocks):
                low = (zb * blocks + j) * LANES
                centre_ref[zp * ROWS : (zp + 1) * ROWS, low : low + LANES] = all_ref[
                    zp * HALVES + zb, j * ROWS : (j + 1) * ROWS, :
                ]
    share = LANES // ROWS
    for t in range(SIDE // share):
        first = t * share * HALVES
        denom = jnp.maximum(all_ref[first, tail : tail + 1, :], 1.0)
        squares = sum(all_ref[first + zb, tail + 1 : tail + 2, :] for zb in range(HALVES))
        norm = sum(all_ref[first + k, tail + 2 : tail + 3, :] for k in range(share * HALVES))
        spread_ref[t : t + 1, :] = (squares - norm / denom) / (denom * width)


def lay(gathered, width):
    return pl.pallas_call(
        lay_kernel,
        out_shape=[
            jax.ShapeDtypeStruct((CL_OWN, width), jnp.float32),
            jax.ShapeDtypeStruct((CL_OWN // LANES, LANES), jnp.float32),
        ],
        in_specs=[whole()],
        out_specs=[whole(), whole()],
        compiler_params=params(6),
        name="lay",
    )(gathered)


def body(points, assignment):
    rows, width = points.shape
    owner = assignment >> 8
    label = assignment & (CL_OWN - 1)
    slot = ((owner >> 4) * 4 + (owner & 3)) * SIDE + ((owner >> 2) & 3)
    matches = slot[:, None] == jnp.arange(OWNERS, dtype=jnp.int32)[None, :]
    matches = matches.astype(jnp.float32)
    earlier = (jnp.arange(rows)[:, None] > jnp.arange(rows)[None, :]).astype(jnp.float32)
    before = jnp.dot(earlier, matches, preferred_element_type=jnp.float32)
    position = jnp.sum(before * matches, axis=1).astype(jnp.int32)
    stride = width // LANES // HALVES * SLOTS + TAIL
    row = (slot // SIDE) * stride + (slot % SIDE) * CAP + position
    at = position[:, None] == jnp.arange(CAP, dtype=jnp.int32)[None, :]
    placed = lax.dot_general(
        matches,
        jnp.where(at, (label + 1).astype(jnp.float32)[:, None], 0.0),
        (((0,), (0,)), ((), ())),
        preferred_element_type=jnp.float32,
    )
    share = LANES // CAP
    group = (lax.axis_index("yb") * 2 + lax.axis_index("c")) % share
    lanes = jnp.arange(LANES, dtype=jnp.int32)[None, None, :] // CAP == group
    tags = jnp.where(lanes, jnp.tile(placed.reshape(GROUPS, SIDE, CAP), (1, 1, share)), 0.0)
    tags = jnp.pad(tags, ((0, 0), (0, TAIL - SIDE), (0, 0)))

    packed = pack(row, points, tags)
    met = lax.all_to_all(packed, ("zb", "x", "yb", "c"), split_axis=0, concat_axis=0, tiled=True)
    partial = merge(met)
    partial = lax.all_to_all(partial, ("yp", "zp"), split_axis=0, concat_axis=0, tiled=True)
    offset = (lax.axis_index("zp") * ROWS % LANES).reshape(1)
    done = finish(offset, partial)
    gathered = lax.all_gather(done, ("zp", "zb"), axis=0, tiled=False)
    centre, spread = lay(gathered, width)
    return centre, spread.reshape(CL_OWN)


def solution(mesh):
    fine = Mesh(mesh.devices.reshape(4, 2, 4, 4, 2, 2), ("zp", "zb", "x", "yp", "yb", "c"))
    every = ("zp", "zb", "x", "yp", "yb", "c")
    owners = ("x", "yp", "yb", "c")
    return jax.shard_map(
        body,
        mesh=fine,
        in_specs=(P(every, None), P(every)),
        out_specs=(P(owners, None), P(owners)),
        check_vma=False,
    )
```

```python
import jax
import jax.numpy as jnp
from jax import lax
from jax.experimental import pallas as pl
from jax.experimental.pallas import tpu as pltpu
from jax.sharding import Mesh
from jax.sharding import PartitionSpec as P

CL_OWN = 256
OWNERS = 64
LANES = 128
CAP = 32
SIDE = 4
GROUPS = OWNERS // SIDE
HALVES = 2
MERGE = GROUPS * HALVES
SLOTS = SIDE * CAP
ROWS = CL_OWN // SIDE
KEYS = MERGE * CAP
TAIL = 8
PIECES = 4


def split3(value):
    first = value.astype(jnp.bfloat16)
    rest = value - first.astype(jnp.float32)
    second = rest.astype(jnp.bfloat16)
    third = (rest - second.astype(jnp.float32)).astype(jnp.bfloat16)
    return first, second, third


def whole(space=pltpu.VMEM):
    return pl.BlockSpec(memory_space=space)


def params(mib):
    return pltpu.CompilerParams(vmem_limit_bytes=mib * 1024 * 1024)


def pack_kernel(row_ref, given_ref, tags_ref, out_ref, points_ref, sems):
    rows, width = points_ref.shape
    piece = rows // PIECES
    copies = [
        pltpu.make_async_copy(
            given_ref.at[pl.ds(k * piece, piece)], points_ref.at[pl.ds(k * piece, piece)], sems.at[k]
        )
        for k in range(PIECES)
    ]
    for copy in copies:
        copy.start()
    blocks = width // LANES // HALVES
    stride = blocks * SLOTS + TAIL
    flat = out_ref.reshape(MERGE * stride, LANES)

    def clear(g, carry):
        start = pl.multiple_of(g * stride, 8)
        flat[pl.ds(start, stride - TAIL), :] = jnp.zeros((stride - TAIL, LANES), jnp.float32)
        flat[pl.ds(start + stride - TAIL, TAIL), :] = tags_ref[g & (GROUPS - 1)]
        return carry

    lax.fori_loop(0, MERGE, clear, 0)

    def place(i, carry):
        start = pl.multiple_of(i * 8, 8)
        ats = [row_ref[i * 8 + r] for r in range(8)]
        for h in range(HALVES):
            for j in range(blocks):
                low = (h * blocks + j) * LANES
                tile = points_ref[pl.ds(start, 8), low : low + LANES]
                for r in range(8):
                    at = ats[r] + (h * GROUPS * stride + j * SLOTS)
                    flat[pl.ds(at, 1), :] = tile[r : r + 1]
        return carry

    for k, copy in enumerate(copies):
        copy.wait()
        lax.fori_loop(k * piece // 8, (k + 1) * piece // 8, place, 0)


def pack(row, points, tags):
    blocks = points.shape[1] // LANES // HALVES
    return pl.pallas_call(
        pack_kernel,
        out_shape=jax.ShapeDtypeStruct((MERGE, blocks * SLOTS + TAIL, LANES), jnp.float32),
        in_specs=[whole(pltpu.SMEM), whole(pltpu.HBM), whole()],
        out_specs=whole(),
        scratch_shapes=[
            pltpu.VMEM(points.shape, jnp.float32),
            pltpu.SemaphoreType.DMA((PIECES,)),
        ],
        compiler_params=params(12),
        name="pack",
    )(row, points, tags)


def merge_kernel(arrived_ref, out_ref, hot_ref, square_ref):
    blocks = (arrived_ref.shape[1] - TAIL) // SLOTS
    tail = blocks * SLOTS
    gather = LANES // CAP
    tiles = []
    for k in range(MERGE // gather):
        tile = arrived_ref[k * gather, tail:, :]
        for s in range(1, gather):
            tile = tile + arrived_ref[k * gather + s, tail:, :]
        tiles.append(tile)
    tags = jnp.concatenate(tiles, axis=1).astype(jnp.int32)
    cluster = lax.broadcasted_iota(jnp.int32, (CL_OWN, KEYS), 0) + 1
    for m in range(SIDE):
        hot = (cluster == tags[m : m + 1]).astype(jnp.float32).astype(jnp.bfloat16)
        hot_ref[m] = hot
        for j in range(blocks):
            low = j * SLOTS + m * CAP
            data = arrived_ref[:, low : low + CAP, :].reshape(KEYS, LANES)
            squares = data * data
            square_ref[...] = squares if j == 0 else square_ref[...] + squares
            terms = jnp.concatenate(split3(data), axis=1)
            total = jnp.dot(hot_ref[m], terms, preferred_element_type=jnp.float32)
            total = total[:, 2 * LANES :] + total[:, LANES : 2 * LANES] + total[:, :LANES]
            for zp in range(SIDE):
                out_ref[m * SIDE + zp, j * ROWS : (j + 1) * ROWS, :] = total[
                    zp * ROWS : (zp + 1) * ROWS
                ]
        ones = jnp.ones((TAIL, LANES), jnp.bfloat16)
        norms = sum(
            lax.dot_general(
                ones, term, (((1,), (1,)), ((), ())), preferred_element_type=jnp.float32
            )
            for term in reversed(split3(square_ref[...]))
        )
        row = lax.broadcasted_iota(jnp.int32, (TAIL, KEYS), 0)
        values = jnp.where(row == 0, 1.0, 0.0)
        for k, term in enumerate(split3(norms), 1):
            values = jnp.where(row == k, term.astype(jnp.float32), values)
        small = lax.dot_general(
            values.astype(jnp.bfloat16),
            hot_ref[m],
            (((1,), (1,)), ((), ())),
            preferred_element_type=jnp.float32,
        )
        for zp in range(SIDE):
            low = zp * ROWS // LANES * LANES
            out_ref[m * SIDE + zp, blocks * ROWS :, :] = small[:, low : low + LANES]


def merge(arrived):
    blocks = (arrived.shape[1] - TAIL) // SLOTS
    return pl.pallas_call(
        merge_kernel,
        out_shape=jax.ShapeDtypeStruct((SIDE * SIDE, blocks * ROWS + TAIL, LANES), jnp.float32),
        in_specs=[whole()],
        out_specs=whole(),
        scratch_shapes=[
            pltpu.VMEM((SIDE, CL_OWN, KEYS), jnp.bfloat16),
            pltpu.VMEM((KEYS, LANES), jnp.float32),
        ],
        compiler_params=params(16),
        name="merge",
    )(arrived)


def add_kernel(arrived_ref, out_ref):
    out_ref[...] = (arrived_ref[0] + arrived_ref[1]) + (arrived_ref[2] + arrived_ref[3])


def add(arrived):
    return pl.pallas_call(
        add_kernel,
        out_shape=jax.ShapeDtypeStruct(arrived.shape[1:], jnp.float32),
        in_specs=[whole()],
        out_specs=whole(),
        compiler_params=params(6),
        name="add",
    )(arrived)


def finish_kernel(offset_ref, arrived_ref, out_ref):
    total = (arrived_ref[0] + arrived_ref[1]) + (arrived_ref[2] + arrived_ref[3])
    tail = total.shape[0] - TAIL
    row = lax.broadcasted_iota(jnp.int32, (ROWS, LANES), 0)
    lane = lax.broadcasted_iota(jnp.int32, (ROWS, LANES), 1)
    mine = lane == row + offset_ref[0]
    counts = jnp.sum(jnp.where(mine, total[tail : tail + 1], 0.0), axis=1, keepdims=True)
    denom = jnp.maximum(counts, 1.0)
    norm = jnp.zeros((ROWS, LANES), jnp.float32)
    for low in range(0, tail, ROWS):
        sums = total[low : low + ROWS]
        norm = norm + sums * sums
        means = sums / denom
        for k in range(out_ref.shape[0]):
            out_ref[k, low : low + ROWS, :] = means
    norm = jnp.sum(norm, axis=1, keepdims=True)
    norm = jnp.sum(jnp.where(mine, norm, 0.0), axis=0, keepdims=True)
    squares = total[tail + 1 : tail + 2] + total[tail + 2 : tail + 3] + total[tail + 3 : tail + 4]
    line = lax.broadcasted_iota(jnp.int32, (TAIL, LANES), 0)
    last = jnp.where(line == 0, total[tail : tail + 1], 0.0)
    last = jnp.where(line == 1, squares, last)
    last = jnp.where(line == 2, norm, last)
    for k in range(out_ref.shape[0]):
        out_ref[k, tail:, :] = last


def finish(offset, arrived):
    return pl.pallas_call(
        finish_kernel,
        out_shape=jax.ShapeDtypeStruct((SIDE * HALVES, *arrived.shape[1:]), jnp.float32),
        in_specs=[whole(pltpu.SMEM), whole()],
        out_specs=whole(),
        compiler_params=params(6),
        name="finish",
    )(offset, arrived)


def lay_kernel(all_ref, centre_ref, spread_ref):
    width = centre_ref.shape[1]
    blocks = width // LANES // HALVES
    tail = blocks * ROWS
    for zp in range(SIDE):
        for zb in range(HALVES):
            for j in range(blocks):
                low = (zb * blocks + j) * LANES
                centre_ref[zp * ROWS : (zp + 1) * ROWS, low : low + LANES] = all_ref[
                    zp * HALVES + zb, j * ROWS : (j + 1) * ROWS, :
                ]
    share = LANES // ROWS
    for t in range(SIDE // share):
        first = t * share * HALVES
        denom = jnp.maximum(all_ref[first, tail : tail + 1, :], 1.0)
        squares = sum(all_ref[first + zb, tail + 1 : tail + 2, :] for zb in range(HALVES))
        norm = sum(all_ref[first + k, tail + 2 : tail + 3, :] for k in range(share * HALVES))
        spread_ref[t : t + 1, :] = (squares - norm / denom) / (denom * width)


def lay(gathered, width):
    return pl.pallas_call(
        lay_kernel,
        out_shape=[
            jax.ShapeDtypeStruct((CL_OWN, width), jnp.float32),
            jax.ShapeDtypeStruct((CL_OWN // LANES, LANES), jnp.float32),
        ],
        in_specs=[whole()],
        out_specs=[whole(), whole()],
        compiler_params=params(6),
        name="lay",
    )(gathered)


def body(points, assignment):
    rows, width = points.shape
    owner = assignment >> 8
    label = assignment & (CL_OWN - 1)
    slot = ((owner >> 4) * 4 + (owner & 3)) * SIDE + ((owner >> 2) & 3)
    matches = slot[:, None] == jnp.arange(OWNERS, dtype=jnp.int32)[None, :]
    matches = matches.astype(jnp.float32)
    earlier = (jnp.arange(rows)[:, None] > jnp.arange(rows)[None, :]).astype(jnp.float32)
    before = jnp.dot(earlier, matches, preferred_element_type=jnp.float32)
    position = jnp.sum(before * matches, axis=1).astype(jnp.int32)
    stride = width // LANES // HALVES * SLOTS + TAIL
    row = (slot // SIDE) * stride + (slot % SIDE) * CAP + position
    at = position[:, None] == jnp.arange(CAP, dtype=jnp.int32)[None, :]
    placed = lax.dot_general(
        matches,
        jnp.where(at, (label + 1).astype(jnp.float32)[:, None], 0.0),
        (((0,), (0,)), ((), ())),
        preferred_element_type=jnp.float32,
    )
    share = LANES // CAP
    group = (lax.axis_index("yb") * 2 + lax.axis_index("c")) % share
    lanes = jnp.arange(LANES, dtype=jnp.int32)[None, None, :] // CAP == group
    tags = jnp.where(lanes, jnp.tile(placed.reshape(GROUPS, SIDE, CAP), (1, 1, share)), 0.0)
    tags = jnp.pad(tags, ((0, 0), (0, TAIL - SIDE), (0, 0)))

    packed = pack(row, points, tags)
    met = lax.all_to_all(packed, ("zb", "x", "yb", "c"), split_axis=0, concat_axis=0, tiled=True)
    partial = merge(met)
    partial = partial.reshape(SIDE, -1, LANES)
    partial = lax.all_to_all(partial, "yp", split_axis=0, concat_axis=0, tiled=True)
    partial = add(partial).reshape(SIDE, -1, LANES)
    partial = lax.all_to_all(partial, "zp", split_axis=0, concat_axis=0, tiled=True)
    offset = (lax.axis_index("zp") * ROWS % LANES).reshape(1)
    done = finish(offset, partial)
    gathered = lax.all_to_all(done, ("zp", "zb"), split_axis=0, concat_axis=0, tiled=True)
    centre, spread = lay(gathered, width)
    return centre, spread.reshape(CL_OWN)


def solution(mesh):
    fine = Mesh(mesh.devices.reshape(4, 2, 4, 4, 2, 2), ("zp", "zb", "x", "yp", "yb", "c"))
    every = ("zp", "zb", "x", "yp", "yb", "c")
    owners = ("x", "yp", "yb", "c")
    return jax.shard_map(
        body,
        mesh=fine,
        in_specs=(P(every, None), P(every)),
        out_specs=(P(owners, None), P(owners)),
        check_vma=False,
    )
```

```python
import jax
import jax.numpy as jnp
from jax import lax
from jax.experimental import pallas as pl
from jax.experimental.pallas import tpu as pltpu
from jax.sharding import Mesh
from jax.sharding import PartitionSpec as P

CL_OWN = 256
OWNERS = 64
LANES = 128
CAP = 32
SIDE = 4
GROUPS = OWNERS // SIDE
HALVES = 2
MERGE = GROUPS * HALVES
SLOTS = SIDE * CAP
ROWS = CL_OWN // SIDE
KEYS = MERGE * CAP
TAIL = 8
PIECES = 4
PACK_MIB = 12


def split3(value):
    first = value.astype(jnp.bfloat16)
    rest = value - first.astype(jnp.float32)
    second = rest.astype(jnp.bfloat16)
    third = (rest - second.astype(jnp.float32)).astype(jnp.bfloat16)
    return first, second, third


def whole(space=pltpu.VMEM):
    return pl.BlockSpec(memory_space=space)


def params(mib):
    return pltpu.CompilerParams(vmem_limit_bytes=mib * 1024 * 1024)


def pack_kernel(group_ref, assignment_ref, given_ref, flat, points_ref, rows_ref, at_ref, sems):
    rows, width = points_ref.shape
    piece = rows // PIECES
    copies = [
        pltpu.make_async_copy(
            given_ref.at[pl.ds(k * piece, piece)], points_ref.at[pl.ds(k * piece, piece)], sems.at[k]
        )
        for k in range(PIECES)
    ]
    for copy in copies:
        copy.start()

    blocks = width // LANES // HALVES
    stride = blocks * SLOTS + TAIL
    earlier = lax.broadcasted_iota(jnp.int32, (LANES, LANES), 0)
    lane = lax.broadcasted_iota(jnp.int32, (LANES, LANES), 1)
    earlier = (earlier < lane).astype(jnp.float32).astype(jnp.bfloat16)
    line = lax.broadcasted_iota(jnp.int32, (OWNERS, LANES), 0)
    place = lax.broadcasted_iota(jnp.int32, (LANES, LANES), 0)
    seen = jnp.zeros((OWNERS, 1), jnp.float32)
    tags = jnp.zeros((OWNERS, LANES), jnp.float32)
    for i in range(rows // LANES):
        assigned = assignment_ref[i : i + 1, :]
        owner = assigned >> 8
        label = (assigned & (CL_OWN - 1)) + 1
        group = (owner >> 4) * 4 + (owner & 3)
        member = (owner >> 2) & 3
        hot = (line == group * SIDE + member).astype(jnp.float32)
        before = jnp.dot(
            hot.astype(jnp.bfloat16), earlier, preferred_element_type=jnp.float32
        )
        position = jnp.sum(hot * (before + seen), axis=0, keepdims=True).astype(jnp.int32)
        seen = seen + jnp.sum(hot, axis=1, keepdims=True)
        rows_ref[i : i + 1, :] = group * stride + member * CAP + position
        at = (place == position + group_ref[0] * CAP).astype(jnp.float32)
        tags = tags + lax.dot_general(
            (hot * label.astype(jnp.float32)).astype(jnp.bfloat16),
            at.astype(jnp.bfloat16),
            (((1,), (1,)), ((), ())),
            preferred_element_type=jnp.float32,
        )
    listing = pltpu.make_async_copy(rows_ref, at_ref, sems.at[PIECES])
    listing.start()

    for g in range(MERGE):
        low = (g + 1) * stride - TAIL
        owners = (g % GROUPS) * SIDE
        flat[low : low + SIDE, :] = tags[owners : owners + SIDE]
        flat[low + SIDE : low + TAIL, :] = jnp.zeros((TAIL - SIDE, LANES), jnp.float32)

    def clear(g, carry):
        start = pl.multiple_of(g * stride, 8)
        flat[pl.ds(start, stride - TAIL), :] = jnp.zeros((stride - TAIL, LANES), jnp.float32)
        return carry

    lax.fori_loop(0, MERGE, clear, 0)
    listing.wait()

    def put(i, carry):
        start = pl.multiple_of(i * 8, 8)
        line = i >> 4
        first = (i & 15) * 8
        ats = [at_ref[line, first + r] for r in range(8)]
        for h in range(HALVES):
            for j in range(blocks):
                low = (h * blocks + j) * LANES
                tile = points_ref[pl.ds(start, 8), low : low + LANES]
                for r in range(8):
                    at = ats[r] + (h * GROUPS * stride + j * SLOTS)
                    flat[pl.ds(at, 1), :] = tile[r : r + 1]
        return carry

    for k, copy in enumerate(copies):
        copy.wait()
        lax.fori_loop(k * piece // 8, (k + 1) * piece // 8, put, 0)


def pack(group, assignment, points):
    rows, width = points.shape
    stride = width // LANES // HALVES * SLOTS + TAIL
    lines = (rows // LANES, LANES)
    packed = pl.pallas_call(
        pack_kernel,
        out_shape=jax.ShapeDtypeStruct((MERGE * stride, LANES), jnp.float32),
        in_specs=[whole(pltpu.SMEM), whole(), whole(pltpu.HBM)],
        out_specs=whole(),
        scratch_shapes=[
            pltpu.VMEM(points.shape, jnp.float32),
            pltpu.VMEM(lines, jnp.int32),
            pltpu.SMEM(lines, jnp.int32),
            pltpu.SemaphoreType.DMA((PIECES + 1,)),
        ],
        compiler_params=params(PACK_MIB),
        name="pack",
    )(group, assignment.reshape(lines), pltpu.with_memory_space_constraint(points, pltpu.HBM))
    return packed.reshape(MERGE, stride, LANES)


def merge_kernel(arrived_ref, out_ref, hot_ref, square_ref):
    blocks = (arrived_ref.shape[1] - TAIL) // SLOTS
    tail = blocks * SLOTS
    gather = LANES // CAP
    tiles = []
    for k in range(MERGE // gather):
        tile = arrived_ref[k * gather, tail:, :]
        for s in range(1, gather):
            tile = tile + arrived_ref[k * gather + s, tail:, :]
        tiles.append(tile)
    tags = jnp.concatenate(tiles, axis=1).astype(jnp.int32)
    cluster = lax.broadcasted_iota(jnp.int32, (CL_OWN, KEYS), 0) + 1
    for m in range(SIDE):
        hot = (cluster == tags[m : m + 1]).astype(jnp.float32).astype(jnp.bfloat16)
        hot_ref[m] = hot
        for j in range(blocks):
            low = j * SLOTS + m * CAP
            data = arrived_ref[:, low : low + CAP, :].reshape(KEYS, LANES)
            squares = data * data
            square_ref[...] = squares if j == 0 else square_ref[...] + squares
            terms = jnp.concatenate(split3(data), axis=1)
            total = jnp.dot(hot_ref[m], terms, preferred_element_type=jnp.float32)
            total = total[:, 2 * LANES :] + total[:, LANES : 2 * LANES] + total[:, :LANES]
            for zp in range(SIDE):
                out_ref[zp * SIDE + m, j * ROWS : (j + 1) * ROWS, :] = total[
                    zp * ROWS : (zp + 1) * ROWS
                ]
        ones = jnp.ones((TAIL, LANES), jnp.bfloat16)
        norms = sum(
            lax.dot_general(
                ones, term, (((1,), (1,)), ((), ())), preferred_element_type=jnp.float32
            )
            for term in reversed(split3(square_ref[...]))
        )
        row = lax.broadcasted_iota(jnp.int32, (TAIL, KEYS), 0)
        values = jnp.where(row == 0, 1.0, 0.0)
        for k, term in enumerate(split3(norms), 1):
            values = jnp.where(row == k, term.astype(jnp.float32), values)
        small = lax.dot_general(
            values.astype(jnp.bfloat16),
            hot_ref[m],
            (((1,), (1,)), ((), ())),
            preferred_element_type=jnp.float32,
        )
        for zp in range(SIDE):
            low = zp * ROWS // LANES * LANES
            out_ref[zp * SIDE + m, blocks * ROWS :, :] = small[:, low : low + LANES]


def merge(arrived):
    blocks = (arrived.shape[1] - TAIL) // SLOTS
    return pl.pallas_call(
        merge_kernel,
        out_shape=jax.ShapeDtypeStruct((SIDE * SIDE, blocks * ROWS + TAIL, LANES), jnp.float32),
        in_specs=[whole()],
        out_specs=whole(),
        scratch_shapes=[
            pltpu.VMEM((SIDE, CL_OWN, KEYS), jnp.bfloat16),
            pltpu.VMEM((KEYS, LANES), jnp.float32),
        ],
        compiler_params=params(16),
        name="merge",
    )(arrived)


def finish_kernel(offset_ref, arrived_ref, out_ref):
    total = arrived_ref[0]
    for k in range(1, SIDE * SIDE):
        total = total + arrived_ref[k]
    tail = total.shape[0] - TAIL
    row = lax.broadcasted_iota(jnp.int32, (ROWS, LANES), 0)
    lane = lax.broadcasted_iota(jnp.int32, (ROWS, LANES), 1)
    mine = lane == row + offset_ref[0]
    counts = jnp.sum(jnp.where(mine, total[tail : tail + 1], 0.0), axis=1, keepdims=True)
    denom = jnp.maximum(counts, 1.0)
    norm = jnp.zeros((ROWS, LANES), jnp.float32)
    for low in range(0, tail, ROWS):
        sums = total[low : low + ROWS]
        norm = norm + sums * sums
        out_ref[low : low + ROWS, :] = sums / denom
    norm = jnp.sum(norm, axis=1, keepdims=True)
    norm = jnp.sum(jnp.where(mine, norm, 0.0), axis=0, keepdims=True)
    squares = total[tail + 1 : tail + 2] + total[tail + 2 : tail + 3] + total[tail + 3 : tail + 4]
    line = lax.broadcasted_iota(jnp.int32, (TAIL, LANES), 0)
    last = jnp.where(line == 0, total[tail : tail + 1], 0.0)
    last = jnp.where(line == 1, squares, last)
    out_ref[tail:, :] = jnp.where(line == 2, norm, last)


def finish(offset, arrived):
    return pl.pallas_call(
        finish_kernel,
        out_shape=jax.ShapeDtypeStruct(arrived.shape[1:], jnp.float32),
        in_specs=[whole(pltpu.SMEM), whole()],
        out_specs=whole(),
        compiler_params=params(6),
        name="finish",
    )(offset, arrived)


def lay_kernel(all_ref, centre_ref, spread_ref):
    width = centre_ref.shape[1]
    blocks = width // LANES // HALVES
    tail = blocks * ROWS
    for zp in range(SIDE):
        for zb in range(HALVES):
            for j in range(blocks):
                low = (zb * blocks + j) * LANES
                centre_ref[zp * ROWS : (zp + 1) * ROWS, low : low + LANES] = all_ref[
                    zp * HALVES + zb, j * ROWS : (j + 1) * ROWS, :
                ]
    share = LANES // ROWS
    for t in range(SIDE // share):
        first = t * share * HALVES
        denom = jnp.maximum(all_ref[first, tail : tail + 1, :], 1.0)
        squares = sum(all_ref[first + zb, tail + 1 : tail + 2, :] for zb in range(HALVES))
        norm = sum(all_ref[first + k, tail + 2 : tail + 3, :] for k in range(share * HALVES))
        spread_ref[t : t + 1, :] = (squares - norm / denom) / (denom * width)


def lay(gathered, width):
    return pl.pallas_call(
        lay_kernel,
        out_shape=[
            jax.ShapeDtypeStruct((CL_OWN, width), jnp.float32),
            jax.ShapeDtypeStruct((CL_OWN // LANES, LANES), jnp.float32),
        ],
        in_specs=[whole()],
        out_specs=[whole(), whole()],
        compiler_params=params(6),
        name="lay",
    )(gathered)


def body(points, assignment):
    width = points.shape[1]
    group = (lax.axis_index("yb") * 2 + lax.axis_index("c")) % (LANES // CAP)
    packed = pack(group.reshape(1), assignment, points)
    met = lax.all_to_all(packed, ("zb", "x", "yb", "c"), split_axis=0, concat_axis=0, tiled=True)
    partial = merge(met)
    partial = lax.all_to_all(partial, ("zp", "yp"), split_axis=0, concat_axis=0, tiled=True)
    offset = (lax.axis_index("zp") * ROWS % LANES).reshape(1)
    done = finish(offset, partial)
    gathered = lax.all_gather(done, ("zp", "zb"), axis=0, tiled=False)
    centre, spread = lay(gathered, width)
    return centre, spread.reshape(CL_OWN)


def solution(mesh):
    fine = Mesh(mesh.devices.reshape(4, 2, 4, 4, 2, 2), ("zp", "zb", "x", "yp", "yb", "c"))
    every = ("zp", "zb", "x", "yp", "yb", "c")
    owners = ("x", "yp", "yb", "c")
    return jax.shard_map(
        body,
        mesh=fine,
        in_specs=(P(every, None), P(every)),
        out_specs=(P(owners, None), P(owners)),
        check_vma=False,
    )
```

```python
import jax
import jax.numpy as jnp
from jax import lax
from jax.experimental import pallas as pl
from jax.experimental.pallas import tpu as pltpu
from jax.sharding import Mesh
from jax.sharding import PartitionSpec as P

CL_OWN = 256
OWNERS = 64
LANES = 128
CAP = 32
SIDE = 4
GROUPS = OWNERS // SIDE
HALVES = 2
MERGE = GROUPS * HALVES
SLOTS = SIDE * CAP
ROWS = CL_OWN // SIDE
KEYS = MERGE * CAP
TAIL = 8
PIECES = 2
PACK_MIB = 12


def split3(value):
    first = value.astype(jnp.bfloat16)
    rest = value - first.astype(jnp.float32)
    second = rest.astype(jnp.bfloat16)
    third = (rest - second.astype(jnp.float32)).astype(jnp.bfloat16)
    return first, second, third


def whole(space=pltpu.VMEM):
    return pl.BlockSpec(memory_space=space)


def params(mib):
    return pltpu.CompilerParams(vmem_limit_bytes=mib * 1024 * 1024)


def pack_kernel(group_ref, assignment_ref, given_ref, flat, points_ref, rows_ref, at_ref, sems):
    rows, width = points_ref.shape
    piece = rows // PIECES
    copies = [
        pltpu.make_async_copy(
            given_ref.at[pl.ds(k * piece, piece)], points_ref.at[pl.ds(k * piece, piece)], sems.at[k]
        )
        for k in range(PIECES)
    ]
    for copy in copies:
        copy.start()

    blocks = width // LANES // HALVES
    stride = blocks * SLOTS + TAIL
    earlier = lax.broadcasted_iota(jnp.int32, (LANES, LANES), 0)
    lane = lax.broadcasted_iota(jnp.int32, (LANES, LANES), 1)
    earlier = (earlier < lane).astype(jnp.float32).astype(jnp.bfloat16)
    line = lax.broadcasted_iota(jnp.int32, (OWNERS, LANES), 0)
    place = lax.broadcasted_iota(jnp.int32, (LANES, LANES), 0)
    seen = jnp.zeros((OWNERS, 1), jnp.float32)
    tags = jnp.zeros((OWNERS, LANES), jnp.float32)
    for i in range(rows // LANES):
        assigned = assignment_ref[i : i + 1, :]
        owner = assigned >> 8
        label = (assigned & (CL_OWN - 1)) + 1
        group = (owner >> 4) * 4 + (owner & 3)
        member = (owner >> 2) & 3
        hot = (line == group * SIDE + member).astype(jnp.float32)
        before = jnp.dot(
            hot.astype(jnp.bfloat16), earlier, preferred_element_type=jnp.float32
        )
        position = jnp.sum(hot * (before + seen), axis=0, keepdims=True).astype(jnp.int32)
        seen = seen + jnp.sum(hot, axis=1, keepdims=True)
        rows_ref[i : i + 1, :] = group * stride + member * CAP + position
        at = (place == position + group_ref[0] * CAP).astype(jnp.float32)
        tags = tags + lax.dot_general(
            (hot * label.astype(jnp.float32)).astype(jnp.bfloat16),
            at.astype(jnp.bfloat16),
            (((1,), (1,)), ((), ())),
            preferred_element_type=jnp.float32,
        )
    listing = pltpu.make_async_copy(rows_ref, at_ref, sems.at[PIECES])
    listing.start()

    for g in range(MERGE):
        low = (g + 1) * stride - TAIL
        owners = (g % GROUPS) * SIDE
        flat[low : low + SIDE, :] = tags[owners : owners + SIDE]
        flat[low + SIDE : low + TAIL, :] = jnp.zeros((TAIL - SIDE, LANES), jnp.float32)

    def clear(g, carry):
        start = pl.multiple_of(g * stride, 8)
        flat[pl.ds(start, stride - TAIL), :] = jnp.zeros((stride - TAIL, LANES), jnp.float32)
        return carry

    lax.fori_loop(0, MERGE, clear, 0)
    listing.wait()

    def put(i, carry):
        start = pl.multiple_of(i * LANES, LANES)
        for first in range(0, LANES, 8):
            ats = [at_ref[i, first + r] for r in range(8)]
            for h in range(HALVES):
                for j in range(blocks):
                    low = (h * blocks + j) * LANES
                    tile = points_ref[pl.ds(start + first, 8), low : low + LANES]
                    for r in range(8):
                        at = ats[r] + (h * GROUPS * stride + j * SLOTS)
                        flat[pl.ds(at, 1), :] = tile[r : r + 1]
        return carry

    lines = piece // LANES
    for k, copy in enumerate(copies):
        copy.wait()
        lax.fori_loop(k * lines, (k + 1) * lines, put, 0)


def pack(group, assignment, points):
    rows, width = points.shape
    stride = width // LANES // HALVES * SLOTS + TAIL
    lines = (rows // LANES, LANES)
    packed = pl.pallas_call(
        pack_kernel,
        out_shape=jax.ShapeDtypeStruct((MERGE * stride, LANES), jnp.float32),
        in_specs=[whole(pltpu.SMEM), whole(), whole(pltpu.HBM)],
        out_specs=whole(),
        scratch_shapes=[
            pltpu.VMEM(points.shape, jnp.float32),
            pltpu.VMEM(lines, jnp.int32),
            pltpu.SMEM(lines, jnp.int32),
            pltpu.SemaphoreType.DMA((PIECES + 1,)),
        ],
        compiler_params=params(PACK_MIB),
        name="pack",
    )(group, assignment.reshape(lines), pltpu.with_memory_space_constraint(points, pltpu.HBM))
    return packed.reshape(MERGE, stride, LANES)


def merge_kernel(arrived_ref, out_ref, hot_ref, square_ref):
    blocks = (arrived_ref.shape[1] - TAIL) // SLOTS
    tail = blocks * SLOTS
    gather = LANES // CAP
    tiles = []
    for k in range(MERGE // gather):
        tile = arrived_ref[k * gather, tail:, :]
        for s in range(1, gather):
            tile = tile + arrived_ref[k * gather + s, tail:, :]
        tiles.append(tile)
    tags = jnp.concatenate(tiles, axis=1).astype(jnp.int32)
    cluster = lax.broadcasted_iota(jnp.int32, (CL_OWN, KEYS), 0) + 1
    for m in range(SIDE):
        hot = (cluster == tags[m : m + 1]).astype(jnp.float32).astype(jnp.bfloat16)
        hot_ref[m] = hot
        for j in range(blocks):
            low = j * SLOTS + m * CAP
            data = arrived_ref[:, low : low + CAP, :].reshape(KEYS, LANES)
            squares = data * data
            square_ref[...] = squares if j == 0 else square_ref[...] + squares
            terms = jnp.concatenate(split3(data), axis=1)
            total = jnp.dot(hot_ref[m], terms, preferred_element_type=jnp.float32)
            total = total[:, 2 * LANES :] + total[:, LANES : 2 * LANES] + total[:, :LANES]
            for zp in range(SIDE):
                out_ref[m * SIDE + zp, j * ROWS : (j + 1) * ROWS, :] = total[
                    zp * ROWS : (zp + 1) * ROWS
                ]
        ones = jnp.ones((TAIL, LANES), jnp.bfloat16)
        norms = sum(
            lax.dot_general(
                ones, term, (((1,), (1,)), ((), ())), preferred_element_type=jnp.float32
            )
            for term in reversed(split3(square_ref[...]))
        )
        row = lax.broadcasted_iota(jnp.int32, (TAIL, KEYS), 0)
        values = jnp.where(row == 0, 1.0, 0.0)
        for k, term in enumerate(split3(norms), 1):
            values = jnp.where(row == k, term.astype(jnp.float32), values)
        small = lax.dot_general(
            values.astype(jnp.bfloat16),
            hot_ref[m],
            (((1,), (1,)), ((), ())),
            preferred_element_type=jnp.float32,
        )
        for zp in range(SIDE):
            low = zp * ROWS // LANES * LANES
            out_ref[m * SIDE + zp, blocks * ROWS :, :] = small[:, low : low + LANES]


def merge(arrived):
    blocks = (arrived.shape[1] - TAIL) // SLOTS
    return pl.pallas_call(
        merge_kernel,
        out_shape=jax.ShapeDtypeStruct((SIDE * SIDE, blocks * ROWS + TAIL, LANES), jnp.float32),
        in_specs=[whole()],
        out_specs=whole(),
        scratch_shapes=[
            pltpu.VMEM((SIDE, CL_OWN, KEYS), jnp.bfloat16),
            pltpu.VMEM((KEYS, LANES), jnp.float32),
        ],
        compiler_params=params(16),
        name="merge",
    )(arrived)


def finish_kernel(offset_ref, arrived_ref, out_ref):
    total = arrived_ref[0]
    for k in range(1, SIDE * SIDE):
        total = total + arrived_ref[k]
    tail = total.shape[0] - TAIL
    row = lax.broadcasted_iota(jnp.int32, (ROWS, LANES), 0)
    lane = lax.broadcasted_iota(jnp.int32, (ROWS, LANES), 1)
    mine = lane == row + offset_ref[0]
    counts = jnp.sum(jnp.where(mine, total[tail : tail + 1], 0.0), axis=1, keepdims=True)
    denom = jnp.maximum(counts, 1.0)
    norm = jnp.zeros((ROWS, LANES), jnp.float32)
    for low in range(0, tail, ROWS):
        sums = total[low : low + ROWS]
        norm = norm + sums * sums
        out_ref[low : low + ROWS, :] = sums / denom
    norm = jnp.sum(norm, axis=1, keepdims=True)
    norm = jnp.sum(jnp.where(mine, norm, 0.0), axis=0, keepdims=True)
    squares = total[tail + 1 : tail + 2] + total[tail + 2 : tail + 3] + total[tail + 3 : tail + 4]
    line = lax.broadcasted_iota(jnp.int32, (TAIL, LANES), 0)
    last = jnp.where(line == 0, total[tail : tail + 1], 0.0)
    last = jnp.where(line == 1, squares, last)
    out_ref[tail:, :] = jnp.where(line == 2, norm, last)


def finish(offset, arrived):
    return pl.pallas_call(
        finish_kernel,
        out_shape=jax.ShapeDtypeStruct(arrived.shape[1:], jnp.float32),
        in_specs=[whole(pltpu.SMEM), whole()],
        out_specs=whole(),
        compiler_params=params(6),
        name="finish",
    )(offset, arrived)


def lay_kernel(all_ref, centre_ref, spread_ref):
    width = centre_ref.shape[1]
    blocks = width // LANES // HALVES
    tail = blocks * ROWS
    for zp in range(SIDE):
        for zb in range(HALVES):
            for j in range(blocks):
                low = (zb * blocks + j) * LANES
                centre_ref[zp * ROWS : (zp + 1) * ROWS, low : low + LANES] = all_ref[
                    zp * HALVES + zb, j * ROWS : (j + 1) * ROWS, :
                ]
    share = LANES // ROWS
    for t in range(SIDE // share):
        first = t * share * HALVES
        denom = jnp.maximum(all_ref[first, tail : tail + 1, :], 1.0)
        squares = sum(all_ref[first + zb, tail + 1 : tail + 2, :] for zb in range(HALVES))
        norm = sum(all_ref[first + k, tail + 2 : tail + 3, :] for k in range(share * HALVES))
        spread_ref[t : t + 1, :] = (squares - norm / denom) / (denom * width)


def lay(gathered, width):
    return pl.pallas_call(
        lay_kernel,
        out_shape=[
            jax.ShapeDtypeStruct((CL_OWN, width), jnp.float32),
            jax.ShapeDtypeStruct((CL_OWN // LANES, LANES), jnp.float32),
        ],
        in_specs=[whole()],
        out_specs=[whole(), whole()],
        compiler_params=params(6),
        name="lay",
    )(gathered)


def body(points, assignment):
    width = points.shape[1]
    group = (lax.axis_index("yb") * 2 + lax.axis_index("c")) % (LANES // CAP)
    packed = pack(group.reshape(1), assignment, points)
    met = lax.all_to_all(packed, ("zb", "x", "yb", "c"), split_axis=0, concat_axis=0, tiled=True)
    partial = merge(met)
    partial = lax.all_to_all(partial, ("yp", "zp"), split_axis=0, concat_axis=0, tiled=True)
    offset = (lax.axis_index("zp") * ROWS % LANES).reshape(1)
    done = finish(offset, partial)
    gathered = lax.all_gather(done, ("zp", "zb"), axis=0, tiled=False)
    centre, spread = lay(gathered, width)
    return centre, spread.reshape(CL_OWN)


def solution(mesh):
    fine = Mesh(mesh.devices.reshape(4, 2, 4, 4, 2, 2), ("zp", "zb", "x", "yp", "yb", "c"))
    every = ("zp", "zb", "x", "yp", "yb", "c")
    owners = ("x", "yp", "yb", "c")
    return jax.shard_map(
        body,
        mesh=fine,
        in_specs=(P(every, None), P(every)),
        out_specs=(P(owners, None), P(owners)),
        check_vma=False,
    )
```

```python
import jax
import jax.numpy as jnp
from jax import lax
from jax.experimental import pallas as pl
from jax.experimental.pallas import tpu as pltpu
from jax.sharding import Mesh
from jax.sharding import PartitionSpec as P

CL_OWN = 256
OWNERS = 64
LANES = 128
CAP = 32
SIDE = 4
GROUPS = OWNERS // SIDE
HALVES = 2
MERGE = GROUPS * HALVES
SLOTS = SIDE * CAP
ROWS = CL_OWN // SIDE
KEYS = MERGE * CAP
TAIL = 8
PIECES = 2
PACK_MIB = 12


def split3(value):
    first = value.astype(jnp.bfloat16)
    rest = value - first.astype(jnp.float32)
    second = rest.astype(jnp.bfloat16)
    third = (rest - second.astype(jnp.float32)).astype(jnp.bfloat16)
    return first, second, third


def whole(space=pltpu.VMEM):
    return pl.BlockSpec(memory_space=space)


def params(mib):
    return pltpu.CompilerParams(vmem_limit_bytes=mib * 1024 * 1024)


def pack_kernel(here_ref, assignment_ref, given_ref, flat, points_ref, rows_ref, at_ref, sems):
    rows, width = points_ref.shape
    piece = rows // PIECES
    copies = [
        pltpu.make_async_copy(
            given_ref.at[pl.ds(k * piece, piece)], points_ref.at[pl.ds(k * piece, piece)], sems.at[k]
        )
        for k in range(PIECES)
    ]
    for copy in copies:
        copy.start()

    blocks = width // LANES // HALVES
    stride = blocks * SLOTS + TAIL
    earlier = lax.broadcasted_iota(jnp.int32, (LANES, LANES), 0)
    lane = lax.broadcasted_iota(jnp.int32, (LANES, LANES), 1)
    earlier = (earlier < lane).astype(jnp.float32).astype(jnp.bfloat16)
    line = lax.broadcasted_iota(jnp.int32, (OWNERS, LANES), 0)
    place = lax.broadcasted_iota(jnp.int32, (LANES, LANES), 0)
    seen = jnp.zeros((OWNERS, 1), jnp.float32)
    tags = jnp.zeros((OWNERS, LANES), jnp.float32)
    for i in range(rows // LANES):
        assigned = assignment_ref[i : i + 1, :]
        owner = assigned >> 8
        label = (assigned & (CL_OWN - 1)) + 1
        group = (owner >> 4) * 4 + (owner & 3)
        member = (owner >> 2) & 3
        hot = (line == group * SIDE + member).astype(jnp.float32)
        before = jnp.dot(
            hot.astype(jnp.bfloat16), earlier, preferred_element_type=jnp.float32
        )
        position = jnp.sum(hot * (before + seen), axis=0, keepdims=True).astype(jnp.int32)
        seen = seen + jnp.sum(hot, axis=1, keepdims=True)
        rows_ref[i : i + 1, :] = group * stride + member * CAP + position
        at = (place == position + (here_ref[0] >> 7) * CAP).astype(jnp.float32)
        tags = tags + lax.dot_general(
            (hot * label.astype(jnp.float32)).astype(jnp.bfloat16),
            at.astype(jnp.bfloat16),
            (((1,), (1,)), ((), ())),
            preferred_element_type=jnp.float32,
        )
    listing = pltpu.make_async_copy(rows_ref, at_ref, sems.at[PIECES])
    listing.start()

    for g in range(MERGE):
        low = (g + 1) * stride - TAIL
        owners = (g % GROUPS) * SIDE
        flat[low : low + SIDE, :] = tags[owners : owners + SIDE]
        flat[low + SIDE : low + TAIL, :] = jnp.zeros((TAIL - SIDE, LANES), jnp.float32)

    def clear(g, carry):
        start = pl.multiple_of(g * stride, 8)
        flat[pl.ds(start, stride - TAIL), :] = jnp.zeros((stride - TAIL, LANES), jnp.float32)
        return carry

    lax.fori_loop(0, MERGE, clear, 0)
    listing.wait()

    def put(i, carry):
        start = pl.multiple_of(i * LANES, LANES)
        for first in range(0, LANES, 8):
            ats = [at_ref[i, first + r] for r in range(8)]
            for h in range(HALVES):
                for j in range(blocks):
                    low = (h * blocks + j) * LANES
                    tile = points_ref[pl.ds(start + first, 8), low : low + LANES]
                    for r in range(8):
                        at = ats[r] + (h * GROUPS * stride + j * SLOTS)
                        flat[pl.ds(at, 1), :] = tile[r : r + 1]
        return carry

    lines = piece // LANES
    for k, copy in enumerate(copies):
        copy.wait()
        lax.fori_loop(k * lines, (k + 1) * lines, put, 0)


def pack(here, assignment, points):
    rows, width = points.shape
    stride = width // LANES // HALVES * SLOTS + TAIL
    lines = (rows // LANES, LANES)
    packed = pl.pallas_call(
        pack_kernel,
        out_shape=jax.ShapeDtypeStruct((MERGE * stride, LANES), jnp.float32),
        in_specs=[whole(pltpu.SMEM), whole(), whole(pltpu.HBM)],
        out_specs=whole(),
        scratch_shapes=[
            pltpu.VMEM(points.shape, jnp.float32),
            pltpu.VMEM(lines, jnp.int32),
            pltpu.SMEM(lines, jnp.int32),
            pltpu.SemaphoreType.DMA((PIECES + 1,)),
        ],
        compiler_params=params(PACK_MIB),
        name="pack",
    )(here, assignment.reshape(lines), pltpu.with_memory_space_constraint(points, pltpu.HBM))
    return packed.reshape(MERGE, stride, LANES)


def merge_kernel(arrived_ref, out_ref, hot_ref, square_ref):
    blocks = (arrived_ref.shape[1] - TAIL) // SLOTS
    tail = blocks * SLOTS
    gather = LANES // CAP
    tiles = []
    for k in range(MERGE // gather):
        tile = arrived_ref[k * gather, tail:, :]
        for s in range(1, gather):
            tile = tile + arrived_ref[k * gather + s, tail:, :]
        tiles.append(tile)
    tags = jnp.concatenate(tiles, axis=1).astype(jnp.int32)
    cluster = lax.broadcasted_iota(jnp.int32, (CL_OWN, KEYS), 0) + 1
    for m in range(SIDE):
        hot = (cluster == tags[m : m + 1]).astype(jnp.float32).astype(jnp.bfloat16)
        hot_ref[m] = hot
        for j in range(blocks):
            low = j * SLOTS + m * CAP
            data = arrived_ref[:, low : low + CAP, :].reshape(KEYS, LANES)
            squares = data * data
            square_ref[...] = squares if j == 0 else square_ref[...] + squares
            terms = jnp.concatenate(split3(data), axis=1)
            total = jnp.dot(hot_ref[m], terms, preferred_element_type=jnp.float32)
            total = total[:, 2 * LANES :] + total[:, LANES : 2 * LANES] + total[:, :LANES]
            for zp in range(SIDE):
                out_ref[m * SIDE + zp, j * ROWS : (j + 1) * ROWS, :] = total[
                    zp * ROWS : (zp + 1) * ROWS
                ]
        ones = jnp.ones((TAIL, LANES), jnp.bfloat16)
        norms = sum(
            lax.dot_general(
                ones, term, (((1,), (1,)), ((), ())), preferred_element_type=jnp.float32
            )
            for term in reversed(split3(square_ref[...]))
        )
        row = lax.broadcasted_iota(jnp.int32, (TAIL, KEYS), 0)
        values = jnp.where(row == 0, 1.0, 0.0)
        for k, term in enumerate(split3(norms), 1):
            values = jnp.where(row == k, term.astype(jnp.float32), values)
        small = lax.dot_general(
            values.astype(jnp.bfloat16),
            hot_ref[m],
            (((1,), (1,)), ((), ())),
            preferred_element_type=jnp.float32,
        )
        for zp in range(SIDE):
            low = zp * ROWS // LANES * LANES
            out_ref[m * SIDE + zp, blocks * ROWS :, :] = small[:, low : low + LANES]


def merge(arrived):
    blocks = (arrived.shape[1] - TAIL) // SLOTS
    return pl.pallas_call(
        merge_kernel,
        out_shape=jax.ShapeDtypeStruct((SIDE * SIDE, blocks * ROWS + TAIL, LANES), jnp.float32),
        in_specs=[whole()],
        out_specs=whole(),
        scratch_shapes=[
            pltpu.VMEM((SIDE, CL_OWN, KEYS), jnp.bfloat16),
            pltpu.VMEM((KEYS, LANES), jnp.float32),
        ],
        compiler_params=params(16),
        name="merge",
    )(arrived)


def finish_kernel(here_ref, arrived_ref, out_ref):
    total = arrived_ref[0]
    for k in range(1, SIDE * SIDE):
        total = total + arrived_ref[k]
    tail = total.shape[0] - TAIL
    row = lax.broadcasted_iota(jnp.int32, (ROWS, LANES), 0)
    lane = lax.broadcasted_iota(jnp.int32, (ROWS, LANES), 1)
    mine = lane == row + (here_ref[0] & (LANES - 1))
    counts = jnp.sum(jnp.where(mine, total[tail : tail + 1], 0.0), axis=1, keepdims=True)
    denom = jnp.maximum(counts, 1.0)
    norm = jnp.zeros((ROWS, LANES), jnp.float32)
    for low in range(0, tail, ROWS):
        sums = total[low : low + ROWS]
        norm = norm + sums * sums
        means = sums / denom
        for k in range(SIDE * HALVES):
            out_ref[k, low : low + ROWS, :] = means
    norm = jnp.sum(norm, axis=1, keepdims=True)
    norm = jnp.sum(jnp.where(mine, norm, 0.0), axis=0, keepdims=True)
    squares = total[tail + 1 : tail + 2] + total[tail + 2 : tail + 3] + total[tail + 3 : tail + 4]
    line = lax.broadcasted_iota(jnp.int32, (TAIL, LANES), 0)
    last = jnp.where(line == 0, total[tail : tail + 1], 0.0)
    last = jnp.where(line == 1, squares, last)
    last = jnp.where(line == 2, norm, last)
    for k in range(SIDE * HALVES):
        out_ref[k, tail:, :] = last


def finish(here, arrived):
    return pl.pallas_call(
        finish_kernel,
        out_shape=jax.ShapeDtypeStruct((SIDE * HALVES, *arrived.shape[1:]), jnp.float32),
        in_specs=[whole(pltpu.SMEM), whole()],
        out_specs=whole(),
        compiler_params=params(6),
        name="finish",
    )(here, arrived)


def lay_kernel(all_ref, centre_ref, spread_ref):
    width = centre_ref.shape[1]
    blocks = width // LANES // HALVES
    tail = blocks * ROWS
    for zp in range(SIDE):
        for zb in range(HALVES):
            for j in range(blocks):
                low = (zb * blocks + j) * LANES
                centre_ref[zp * ROWS : (zp + 1) * ROWS, low : low + LANES] = all_ref[
                    zp * HALVES + zb, j * ROWS : (j + 1) * ROWS, :
                ]
    share = LANES // ROWS
    for t in range(SIDE // share):
        first = t * share * HALVES
        denom = jnp.maximum(all_ref[first, tail : tail + 1, :], 1.0)
        squares = sum(all_ref[first + zb, tail + 1 : tail + 2, :] for zb in range(HALVES))
        norm = sum(all_ref[first + k, tail + 2 : tail + 3, :] for k in range(share * HALVES))
        spread_ref[t : t + 1, :] = (squares - norm / denom) / (denom * width)


def lay(gathered, width):
    return pl.pallas_call(
        lay_kernel,
        out_shape=[
            jax.ShapeDtypeStruct((CL_OWN, width), jnp.float32),
            jax.ShapeDtypeStruct((CL_OWN // LANES, LANES), jnp.float32),
        ],
        in_specs=[whole()],
        out_specs=[whole(), whole()],
        compiler_params=params(6),
        name="lay",
    )(gathered)


def body(points, assignment):
    width = points.shape[1]
    group = (lax.axis_index("yb") * 2 + lax.axis_index("c")) % (LANES // CAP)
    offset = lax.axis_index("zp") * ROWS % LANES
    here = (group * LANES + offset).reshape(1)
    packed = pack(here, assignment, points)
    met = lax.all_to_all(packed, ("zb", "x", "yb", "c"), split_axis=0, concat_axis=0, tiled=True)
    partial = merge(met)
    partial = lax.all_to_all(partial, ("yp", "zp"), split_axis=0, concat_axis=0, tiled=True)
    done = finish(here, partial)
    gathered = lax.all_to_all(done, ("zp", "zb"), split_axis=0, concat_axis=0, tiled=True)
    centre, spread = lay(gathered, width)
    return centre, spread.reshape(CL_OWN)


def solution(mesh):
    fine = Mesh(mesh.devices.reshape(4, 2, 4, 4, 2, 2), ("zp", "zb", "x", "yp", "yb", "c"))
    every = ("zp", "zb", "x", "yp", "yb", "c")
    owners = ("x", "yp", "yb", "c")
    return jax.shard_map(
        body,
        mesh=fine,
        in_specs=(P(every, None), P(every)),
        out_specs=(P(owners, None), P(owners)),
        check_vma=False,
    )
```

```python
import jax
import jax.numpy as jnp
from jax import lax
from jax.experimental import pallas as pl
from jax.experimental.pallas import tpu as pltpu
from jax.sharding import Mesh
from jax.sharding import PartitionSpec as P

CL_OWN = 256
OWNERS = 64
LANES = 128
CAP = 32
SIDE = 4
GROUPS = OWNERS // SIDE
HALVES = 2
MERGE = GROUPS * HALVES
SLOTS = SIDE * CAP
ROWS = CL_OWN // SIDE
KEYS = MERGE * CAP
TAIL = 8
PIECES = 2
PACK_MIB = 12


def split3(value):
    first = value.astype(jnp.bfloat16)
    rest = value - first.astype(jnp.float32)
    second = rest.astype(jnp.bfloat16)
    third = (rest - second.astype(jnp.float32)).astype(jnp.bfloat16)
    return first, second, third


def whole(space=pltpu.VMEM):
    return pl.BlockSpec(memory_space=space)


def params(mib):
    return pltpu.CompilerParams(vmem_limit_bytes=mib * 1024 * 1024)


def pack_kernel(here_ref, assignment_ref, given_ref, flat, points_ref, rows_ref, at_ref, sems):
    rows, width = points_ref.shape
    piece = rows // PIECES
    copies = [
        pltpu.make_async_copy(
            given_ref.at[pl.ds(k * piece, piece)], points_ref.at[pl.ds(k * piece, piece)], sems.at[k]
        )
        for k in range(PIECES)
    ]
    for copy in copies:
        copy.start()

    blocks = width // LANES // HALVES
    stride = blocks * SLOTS + TAIL
    earlier = lax.broadcasted_iota(jnp.int32, (LANES, LANES), 0)
    lane = lax.broadcasted_iota(jnp.int32, (LANES, LANES), 1)
    earlier = (earlier < lane).astype(jnp.float32).astype(jnp.bfloat16)
    line = lax.broadcasted_iota(jnp.int32, (OWNERS, LANES), 0)
    place = lax.broadcasted_iota(jnp.int32, (LANES, LANES), 0)
    seen = jnp.zeros((OWNERS, 1), jnp.float32)
    tags = jnp.zeros((OWNERS, LANES), jnp.float32)
    for i in range(rows // LANES):
        assigned = assignment_ref[i : i + 1, :]
        owner = assigned >> 8
        label = (assigned & (CL_OWN - 1)) + 1
        group = (owner >> 4) * 4 + (owner & 3)
        member = (owner >> 2) & 3
        hot = (line == group * SIDE + member).astype(jnp.float32)
        before = jnp.dot(
            hot.astype(jnp.bfloat16), earlier, preferred_element_type=jnp.float32
        )
        position = jnp.sum(hot * (before + seen), axis=0, keepdims=True).astype(jnp.int32)
        seen = seen + jnp.sum(hot, axis=1, keepdims=True)
        rows_ref[i : i + 1, :] = group * stride + member * CAP + position
        at = (place == position + ((here_ref[0] >> 7) & 3) * CAP).astype(jnp.float32)
        tags = tags + lax.dot_general(
            (hot * label.astype(jnp.float32)).astype(jnp.bfloat16),
            at.astype(jnp.bfloat16),
            (((1,), (1,)), ((), ())),
            preferred_element_type=jnp.float32,
        )
    listing = pltpu.make_async_copy(rows_ref, at_ref, sems.at[PIECES])
    listing.start()

    for g in range(MERGE):
        low = (g + 1) * stride - TAIL
        owners = (g % GROUPS) * SIDE
        flat[low : low + SIDE, :] = tags[owners : owners + SIDE]
        flat[low + SIDE : low + TAIL, :] = jnp.zeros((TAIL - SIDE, LANES), jnp.float32)

    def clear(g, carry):
        start = pl.multiple_of(g * stride, 8)
        flat[pl.ds(start, stride - TAIL), :] = jnp.zeros((stride - TAIL, LANES), jnp.float32)
        return carry

    lax.fori_loop(0, MERGE, clear, 0)
    listing.wait()

    def put(i, carry):
        start = pl.multiple_of(i * LANES, LANES)
        for first in range(0, LANES, 8):
            ats = [at_ref[i, first + r] for r in range(8)]
            for h in range(HALVES):
                for j in range(blocks):
                    low = (h * blocks + j) * LANES
                    tile = points_ref[pl.ds(start + first, 8), low : low + LANES]
                    for r in range(8):
                        at = ats[r] + (h * GROUPS * stride + j * SLOTS)
                        flat[pl.ds(at, 1), :] = tile[r : r + 1]
        return carry

    lines = piece // LANES
    for k, copy in enumerate(copies):
        copy.wait()
        lax.fori_loop(k * lines, (k + 1) * lines, put, 0)


def pack(here, assignment, points):
    rows, width = points.shape
    stride = width // LANES // HALVES * SLOTS + TAIL
    lines = (rows // LANES, LANES)
    packed = pl.pallas_call(
        pack_kernel,
        out_shape=jax.ShapeDtypeStruct((MERGE * stride, LANES), jnp.float32),
        in_specs=[whole(pltpu.SMEM), whole(), whole(pltpu.HBM)],
        out_specs=whole(),
        scratch_shapes=[
            pltpu.VMEM(points.shape, jnp.float32),
            pltpu.VMEM(lines, jnp.int32),
            pltpu.SMEM(lines, jnp.int32),
            pltpu.SemaphoreType.DMA((PIECES + 1,)),
        ],
        compiler_params=params(PACK_MIB),
        name="pack",
    )(here, assignment.reshape(lines), pltpu.with_memory_space_constraint(points, pltpu.HBM))
    return packed.reshape(MERGE, stride, LANES)


def merge_kernel(arrived_ref, out_ref, hot_ref, square_ref):
    blocks = (arrived_ref.shape[1] - TAIL) // SLOTS
    tail = blocks * SLOTS
    gather = LANES // CAP
    tiles = []
    for k in range(MERGE // gather):
        tile = arrived_ref[k * gather, tail:, :]
        for s in range(1, gather):
            tile = tile + arrived_ref[k * gather + s, tail:, :]
        tiles.append(tile)
    tags = jnp.concatenate(tiles, axis=1).astype(jnp.int32)
    cluster = lax.broadcasted_iota(jnp.int32, (CL_OWN, KEYS), 0) + 1
    for m in range(SIDE):
        hot = (cluster == tags[m : m + 1]).astype(jnp.float32).astype(jnp.bfloat16)
        hot_ref[m] = hot
        for j in range(blocks):
            low = j * SLOTS + m * CAP
            data = arrived_ref[:, low : low + CAP, :].reshape(KEYS, LANES)
            squares = data * data
            square_ref[...] = squares if j == 0 else square_ref[...] + squares
            terms = jnp.concatenate(split3(data), axis=1)
            total = jnp.dot(hot_ref[m], terms, preferred_element_type=jnp.float32)
            total = total[:, 2 * LANES :] + total[:, LANES : 2 * LANES] + total[:, :LANES]
            for zp in range(SIDE):
                out_ref[m * SIDE + zp, j * ROWS : (j + 1) * ROWS, :] = total[
                    zp * ROWS : (zp + 1) * ROWS
                ]
        ones = jnp.ones((TAIL, LANES), jnp.bfloat16)
        norms = sum(
            lax.dot_general(
                ones, term, (((1,), (1,)), ((), ())), preferred_element_type=jnp.float32
            )
            for term in reversed(split3(square_ref[...]))
        )
        row = lax.broadcasted_iota(jnp.int32, (TAIL, KEYS), 0)
        values = jnp.where(row == 0, 1.0, 0.0)
        for k, term in enumerate(split3(norms), 1):
            values = jnp.where(row == k, term.astype(jnp.float32), values)
        small = lax.dot_general(
            values.astype(jnp.bfloat16),
            hot_ref[m],
            (((1,), (1,)), ((), ())),
            preferred_element_type=jnp.float32,
        )
        for zp in range(SIDE):
            low = zp * ROWS // LANES * LANES
            out_ref[m * SIDE + zp, blocks * ROWS :, :] = small[:, low : low + LANES]


def merge(arrived):
    blocks = (arrived.shape[1] - TAIL) // SLOTS
    return pl.pallas_call(
        merge_kernel,
        out_shape=jax.ShapeDtypeStruct((SIDE * SIDE, blocks * ROWS + TAIL, LANES), jnp.float32),
        in_specs=[whole()],
        out_specs=whole(),
        scratch_shapes=[
            pltpu.VMEM((SIDE, CL_OWN, KEYS), jnp.bfloat16),
            pltpu.VMEM((KEYS, LANES), jnp.float32),
        ],
        compiler_params=params(16),
        name="merge",
    )(arrived)


def finish_kernel(here_ref, arrived_ref, out_ref):
    total = arrived_ref[0]
    for k in range(1, SIDE * SIDE):
        total = total + arrived_ref[k]
    tail = total.shape[0] - TAIL
    row = lax.broadcasted_iota(jnp.int32, (ROWS, LANES), 0)
    lane = lax.broadcasted_iota(jnp.int32, (ROWS, LANES), 1)
    mine = lane == row + (here_ref[0] & (LANES - 1))
    counts = jnp.sum(jnp.where(mine, total[tail : tail + 1], 0.0), axis=1, keepdims=True)
    denom = jnp.maximum(counts, 1.0)
    norm = jnp.zeros((ROWS, LANES), jnp.float32)
    for low in range(0, tail, ROWS):
        sums = total[low : low + ROWS]
        norm = norm + sums * sums
        out_ref[low : low + ROWS, :] = sums / denom
    norm = jnp.sum(norm, axis=1, keepdims=True)
    norm = jnp.sum(jnp.where(mine, norm, 0.0), axis=0, keepdims=True)
    squares = total[tail + 1 : tail + 2] + total[tail + 2 : tail + 3] + total[tail + 3 : tail + 4]
    line = lax.broadcasted_iota(jnp.int32, (TAIL, LANES), 0)
    last = jnp.where(line == 0, total[tail : tail + 1], 0.0)
    last = jnp.where(line == 1, squares, last)
    out_ref[tail:, :] = jnp.where(line == 2, norm, last)


def finish(here, arrived):
    return pl.pallas_call(
        finish_kernel,
        out_shape=jax.ShapeDtypeStruct(arrived.shape[1:], jnp.float32),
        in_specs=[whole(pltpu.SMEM), whole()],
        out_specs=whole(),
        compiler_params=params(6),
        name="finish",
    )(here, arrived)


def lay_kernel(here_ref, pair_ref, ahead_ref, behind_ref, next_ref, last_ref, centre_ref, spread_ref, tails_ref):
    width = centre_ref.shape[1]
    blocks = width // LANES // HALVES
    tail = blocks * ROWS
    count = SIDE * HALVES
    pieces = [(0, pair_ref, 0), (4, pair_ref, 1), (2, ahead_ref, 0), (6, behind_ref, 0)]
    pieces += [(1, next_ref, 0), (5, next_ref, 1), (7, last_ref, 0), (3, last_ref, 1)]
    for shift, ref, at in pieces:
        z = ((here_ref[0] >> 9) + shift) & (count - 1)
        row = pl.multiple_of((z >> 1) * ROWS, ROWS)
        for j in range(blocks):
            lane = pl.multiple_of(((z & 1) * blocks + j) * LANES, LANES)
            centre_ref[pl.ds(row, ROWS), pl.ds(lane, LANES)] = ref[
                at, j * ROWS : (j + 1) * ROWS, :
            ]
        tails_ref[z] = ref[at, tail:, :]
    share = LANES // ROWS
    for t in range(SIDE // share):
        first = t * share * HALVES
        denom = jnp.maximum(tails_ref[first, 0:1, :], 1.0)
        squares = sum(tails_ref[first + zb, 1:2, :] for zb in range(HALVES))
        norm = sum(tails_ref[first + k, 2:3, :] for k in range(share * HALVES))
        spread_ref[t : t + 1, :] = (squares - norm / denom) / (denom * width)


def lay(here, pieces, width):
    return pl.pallas_call(
        lay_kernel,
        out_shape=[
            jax.ShapeDtypeStruct((CL_OWN, width), jnp.float32),
            jax.ShapeDtypeStruct((CL_OWN // LANES, LANES), jnp.float32),
        ],
        in_specs=[whole(pltpu.SMEM)] + [whole()] * len(pieces),
        out_specs=[whole(), whole()],
        scratch_shapes=[pltpu.VMEM((SIDE * HALVES, TAIL, LANES), jnp.float32)],
        compiler_params=params(6),
        name="lay",
    )(here, *pieces)


def moved(value, by):
    count = SIDE * HALVES
    return lax.ppermute(value, ("zp", "zb"), [((z + by) % count, z) for z in range(count)])


def body(points, assignment):
    width = points.shape[1]
    group = (lax.axis_index("yb") * 2 + lax.axis_index("c")) % (LANES // CAP)
    offset = lax.axis_index("zp") * ROWS % LANES
    along = lax.axis_index("zp") * HALVES + lax.axis_index("zb")
    here = ((along * (LANES // CAP) + group) * LANES + offset).reshape(1)
    packed = pack(here, assignment, points)
    met = lax.all_to_all(packed, ("zb", "x", "yb", "c"), split_axis=0, concat_axis=0, tiled=True)
    partial = merge(met)
    partial = lax.all_to_all(partial, ("yp", "zp"), split_axis=0, concat_axis=0, tiled=True)
    done = finish(here, partial)
    done = done[None]
    far, ahead, behind = lax.optimization_barrier(tuple(moved(done, by) for by in (4, 2, 6)))
    pair = jnp.concatenate([done, far])
    pieces = (pair, ahead, behind, moved(pair, 1), moved(pair, 7))
    centre, spread = lay(here, pieces, width)
    return centre, spread.reshape(CL_OWN)


def solution(mesh):
    fine = Mesh(mesh.devices.reshape(4, 2, 4, 4, 2, 2), ("zp", "zb", "x", "yp", "yb", "c"))
    every = ("zp", "zb", "x", "yp", "yb", "c")
    owners = ("x", "yp", "yb", "c")
    return jax.shard_map(
        body,
        mesh=fine,
        in_specs=(P(every, None), P(every)),
        out_specs=(P(owners, None), P(owners)),
        check_vma=False,
    )
```

```python
import jax
import jax.numpy as jnp
from jax import lax
from jax.experimental import pallas as pl
from jax.experimental.pallas import tpu as pltpu
from jax.sharding import Mesh
from jax.sharding import PartitionSpec as P

CL_OWN = 256
OWNERS = 64
LANES = 128
CAP = 32
SIDE = 4
GROUPS = OWNERS // SIDE
HALVES = 2
MERGE = GROUPS * HALVES
SLOTS = SIDE * CAP
ROWS = CL_OWN // SIDE
KEYS = MERGE * CAP
TAIL = 8
PIECES = 2
PACK_MIB = 12


def split3(value):
    first = value.astype(jnp.bfloat16)
    rest = value - first.astype(jnp.float32)
    second = rest.astype(jnp.bfloat16)
    third = (rest - second.astype(jnp.float32)).astype(jnp.bfloat16)
    return first, second, third


def whole(space=pltpu.VMEM):
    return pl.BlockSpec(memory_space=space)


def params(mib):
    return pltpu.CompilerParams(vmem_limit_bytes=mib * 1024 * 1024)


def pack_kernel(here_ref, assignment_ref, given_ref, flat, points_ref, rows_ref, at_ref, sems):
    rows, width = points_ref.shape
    piece = rows // PIECES
    copies = [
        pltpu.make_async_copy(
            given_ref.at[pl.ds(k * piece, piece)], points_ref.at[pl.ds(k * piece, piece)], sems.at[k]
        )
        for k in range(PIECES)
    ]
    for copy in copies:
        copy.start()

    blocks = width // LANES // HALVES
    stride = blocks * SLOTS + TAIL
    earlier = lax.broadcasted_iota(jnp.int32, (LANES, LANES), 0)
    lane = lax.broadcasted_iota(jnp.int32, (LANES, LANES), 1)
    earlier = (earlier < lane).astype(jnp.float32).astype(jnp.bfloat16)
    line = lax.broadcasted_iota(jnp.int32, (OWNERS, LANES), 0)
    place = lax.broadcasted_iota(jnp.int32, (LANES, LANES), 0)
    seen = jnp.zeros((OWNERS, 1), jnp.float32)
    tags = jnp.zeros((OWNERS, LANES), jnp.float32)
    for i in range(rows // LANES):
        assigned = assignment_ref[i : i + 1, :]
        owner = assigned >> 8
        label = (assigned & (CL_OWN - 1)) + 1
        group = (owner >> 4) * 4 + (owner & 3)
        member = (owner >> 2) & 3
        hot = (line == group * SIDE + member).astype(jnp.float32)
        before = jnp.dot(
            hot.astype(jnp.bfloat16), earlier, preferred_element_type=jnp.float32
        )
        position = jnp.sum(hot * (before + seen), axis=0, keepdims=True).astype(jnp.int32)
        seen = seen + jnp.sum(hot, axis=1, keepdims=True)
        rows_ref[i : i + 1, :] = group * stride + member * CAP + position
        at = (place == position + (here_ref[0] >> 7) * CAP).astype(jnp.float32)
        tags = tags + lax.dot_general(
            (hot * label.astype(jnp.float32)).astype(jnp.bfloat16),
            at.astype(jnp.bfloat16),
            (((1,), (1,)), ((), ())),
            preferred_element_type=jnp.float32,
        )
    listing = pltpu.make_async_copy(rows_ref, at_ref, sems.at[PIECES])
    listing.start()

    for g in range(MERGE):
        low = (g + 1) * stride - TAIL
        owners = (g % GROUPS) * SIDE
        flat[low : low + SIDE, :] = tags[owners : owners + SIDE]
        flat[low + SIDE : low + TAIL, :] = jnp.zeros((TAIL - SIDE, LANES), jnp.float32)

    def clear(g, carry):
        start = pl.multiple_of(g * stride, 8)
        flat[pl.ds(start, stride - TAIL), :] = jnp.zeros((stride - TAIL, LANES), jnp.float32)
        return carry

    lax.fori_loop(0, MERGE, clear, 0)
    listing.wait()

    def put(i, carry):
        start = pl.multiple_of(i * LANES, LANES)
        for first in range(0, LANES, 8):
            ats = [at_ref[i, first + r] for r in range(8)]
            tiles = [
                points_ref[pl.ds(start + first, 8), k * LANES : (k + 1) * LANES]
                for k in range(HALVES * blocks)
            ]
            for r in range(8):
                for k, tile in enumerate(tiles):
                    at = ats[r] + (k // blocks * GROUPS * stride + k % blocks * SLOTS)
                    flat[pl.ds(at, 1), :] = tile[r : r + 1]
        return carry

    lines = piece // LANES
    for k, copy in enumerate(copies):
        copy.wait()
        lax.fori_loop(k * lines, (k + 1) * lines, put, 0)


def pack(here, assignment, points):
    rows, width = points.shape
    stride = width // LANES // HALVES * SLOTS + TAIL
    lines = (rows // LANES, LANES)
    packed = pl.pallas_call(
        pack_kernel,
        out_shape=jax.ShapeDtypeStruct((MERGE * stride, LANES), jnp.float32),
        in_specs=[whole(pltpu.SMEM), whole(), whole(pltpu.HBM)],
        out_specs=whole(),
        scratch_shapes=[
            pltpu.VMEM(points.shape, jnp.float32),
            pltpu.VMEM(lines, jnp.int32),
            pltpu.SMEM(lines, jnp.int32),
            pltpu.SemaphoreType.DMA((PIECES + 1,)),
        ],
        compiler_params=params(PACK_MIB),
        name="pack",
    )(here, assignment.reshape(lines), pltpu.with_memory_space_constraint(points, pltpu.HBM))
    return packed.reshape(MERGE, stride, LANES)


def merge_kernel(arrived_ref, out_ref, hot_ref, square_ref):
    blocks = (arrived_ref.shape[1] - TAIL) // SLOTS
    tail = blocks * SLOTS
    gather = LANES // CAP
    tiles = []
    for k in range(MERGE // gather):
        tile = arrived_ref[k * gather, tail:, :]
        for s in range(1, gather):
            tile = tile + arrived_ref[k * gather + s, tail:, :]
        tiles.append(tile)
    tags = jnp.concatenate(tiles, axis=1).astype(jnp.bfloat16)
    cluster = lax.broadcasted_iota(jnp.int32, (CL_OWN, KEYS), 0) + 1
    cluster = cluster.astype(jnp.float32).astype(jnp.bfloat16)
    one = jnp.ones((CL_OWN, KEYS), jnp.bfloat16)
    none = jnp.zeros((CL_OWN, KEYS), jnp.bfloat16)
    for m in range(SIDE):
        hot = jnp.where(cluster == tags[m : m + 1], one, none)
        hot_ref[m] = hot
        for j in range(blocks):
            low = j * SLOTS + m * CAP
            data = arrived_ref[:, low : low + CAP, :].reshape(KEYS, LANES)
            squares = data * data
            square_ref[...] = squares if j == 0 else square_ref[...] + squares
            terms = jnp.concatenate(split3(data)[:2], axis=1)
            total = jnp.dot(hot_ref[m], terms, preferred_element_type=jnp.float32)
            total = total[:, LANES:] + total[:, :LANES]
            for zp in range(SIDE):
                out_ref[m * SIDE + zp, j * ROWS : (j + 1) * ROWS, :] = total[
                    zp * ROWS : (zp + 1) * ROWS
                ]
        ones = jnp.ones((TAIL, LANES), jnp.bfloat16)
        norms = sum(
            lax.dot_general(
                ones, term, (((1,), (1,)), ((), ())), preferred_element_type=jnp.float32
            )
            for term in reversed(split3(square_ref[...]))
        )
        row = lax.broadcasted_iota(jnp.int32, (TAIL, KEYS), 0)
        values = jnp.where(row == 0, 1.0, 0.0)
        for k, term in enumerate(split3(norms), 1):
            values = jnp.where(row == k, term.astype(jnp.float32), values)
        small = lax.dot_general(
            values.astype(jnp.bfloat16),
            hot_ref[m],
            (((1,), (1,)), ((), ())),
            preferred_element_type=jnp.float32,
        )
        for zp in range(SIDE):
            low = zp * ROWS // LANES * LANES
            out_ref[m * SIDE + zp, blocks * ROWS :, :] = small[:, low : low + LANES]


def merge(arrived):
    blocks = (arrived.shape[1] - TAIL) // SLOTS
    return pl.pallas_call(
        merge_kernel,
        out_shape=jax.ShapeDtypeStruct((SIDE * SIDE, blocks * ROWS + TAIL, LANES), jnp.float32),
        in_specs=[whole()],
        out_specs=whole(),
        scratch_shapes=[
            pltpu.VMEM((SIDE, CL_OWN, KEYS), jnp.bfloat16),
            pltpu.VMEM((KEYS, LANES), jnp.float32),
        ],
        compiler_params=params(16),
        name="merge",
    )(arrived)


def finish_kernel(here_ref, arrived_ref, out_ref):
    total = arrived_ref[0]
    for k in range(1, SIDE * SIDE):
        total = total + arrived_ref[k]
    tail = total.shape[0] - TAIL
    row = lax.broadcasted_iota(jnp.int32, (ROWS, LANES), 0)
    lane = lax.broadcasted_iota(jnp.int32, (ROWS, LANES), 1)
    mine = lane == row + (here_ref[0] & (LANES - 1))
    counts = jnp.sum(jnp.where(mine, total[tail : tail + 1], 0.0), axis=1, keepdims=True)
    denom = jnp.maximum(counts, 1.0)
    norm = jnp.zeros((ROWS, LANES), jnp.float32)
    for low in range(0, tail, ROWS):
        sums = total[low : low + ROWS]
        norm = norm + sums * sums
        means = sums / denom
        for k in range(SIDE * HALVES):
            out_ref[k, low : low + ROWS, :] = means
    norm = jnp.sum(norm, axis=1, keepdims=True)
    norm = jnp.sum(jnp.where(mine, norm, 0.0), axis=0, keepdims=True)
    squares = total[tail + 1 : tail + 2] + total[tail + 2 : tail + 3] + total[tail + 3 : tail + 4]
    line = lax.broadcasted_iota(jnp.int32, (TAIL, LANES), 0)
    last = jnp.where(line == 0, total[tail : tail + 1], 0.0)
    last = jnp.where(line == 1, squares, last)
    last = jnp.where(line == 2, norm, last)
    for k in range(SIDE * HALVES):
        out_ref[k, tail:, :] = last


def finish(here, arrived):
    return pl.pallas_call(
        finish_kernel,
        out_shape=jax.ShapeDtypeStruct((SIDE * HALVES, *arrived.shape[1:]), jnp.float32),
        in_specs=[whole(pltpu.SMEM), whole()],
        out_specs=whole(),
        compiler_params=params(6),
        name="finish",
    )(here, arrived)


def lay_kernel(all_ref, centre_ref, spread_ref):
    width = centre_ref.shape[1]
    blocks = width // LANES // HALVES
    tail = blocks * ROWS
    for zp in range(SIDE):
        for zb in range(HALVES):
            for j in range(blocks):
                low = (zb * blocks + j) * LANES
                centre_ref[zp * ROWS : (zp + 1) * ROWS, low : low + LANES] = all_ref[
                    zp * HALVES + zb, j * ROWS : (j + 1) * ROWS, :
                ]
    share = LANES // ROWS
    for t in range(SIDE // share):
        first = t * share * HALVES
        denom = jnp.maximum(all_ref[first, tail : tail + 1, :], 1.0)
        squares = sum(all_ref[first + zb, tail + 1 : tail + 2, :] for zb in range(HALVES))
        norm = sum(all_ref[first + k, tail + 2 : tail + 3, :] for k in range(share * HALVES))
        spread_ref[t : t + 1, :] = (squares - norm / denom) / (denom * width)


def lay(gathered, width):
    return pl.pallas_call(
        lay_kernel,
        out_shape=[
            jax.ShapeDtypeStruct((CL_OWN, width), jnp.float32),
            jax.ShapeDtypeStruct((CL_OWN // LANES, LANES), jnp.float32),
        ],
        in_specs=[whole()],
        out_specs=[whole(), whole()],
        compiler_params=params(6),
        name="lay",
    )(gathered)


def body(points, assignment):
    width = points.shape[1]
    group = (lax.axis_index("yb") * 2 + lax.axis_index("c")) % (LANES // CAP)
    offset = lax.axis_index("zp") * ROWS % LANES
    here = (group * LANES + offset).reshape(1)
    packed = pack(here, assignment, points)
    met = lax.all_to_all(packed, ("zb", "x", "yb", "c"), split_axis=0, concat_axis=0, tiled=True)
    partial = merge(met)
    partial = lax.all_to_all(partial, ("yp", "zp"), split_axis=0, concat_axis=0, tiled=True)
    done = finish(here, partial)
    gathered = lax.all_to_all(done, ("zp", "zb"), split_axis=0, concat_axis=0, tiled=True)
    centre, spread = lay(gathered, width)
    return centre, spread.reshape(CL_OWN)


def solution(mesh):
    fine = Mesh(mesh.devices.reshape(4, 2, 4, 4, 2, 2), ("zp", "zb", "x", "yp", "yb", "c"))
    every = ("zp", "zb", "x", "yp", "yb", "c")
    owners = ("x", "yp", "yb", "c")
    return jax.shard_map(
        body,
        mesh=fine,
        in_specs=(P(every, None), P(every)),
        out_specs=(P(owners, None), P(owners)),
        check_vma=False,
    )
```

```python
import jax
import jax.numpy as jnp
from jax import lax
from jax.experimental import pallas as pl
from jax.experimental.pallas import tpu as pltpu
from jax.sharding import Mesh
from jax.sharding import PartitionSpec as P

CL_OWN = 256
OWNERS = 64
LANES = 128
CAP = 32
SIDE = 4
GROUPS = OWNERS // SIDE
HALVES = 2
MERGE = GROUPS * HALVES
SLOTS = SIDE * CAP
ROWS = CL_OWN // SIDE
KEYS = MERGE * CAP
TAIL = 8
PIECES = 2
PACK_MIB = 12


def split3(value):
    first = value.astype(jnp.bfloat16)
    rest = value - first.astype(jnp.float32)
    second = rest.astype(jnp.bfloat16)
    third = (rest - second.astype(jnp.float32)).astype(jnp.bfloat16)
    return first, second, third


def whole(space=pltpu.VMEM):
    return pl.BlockSpec(memory_space=space)


def params(mib):
    return pltpu.CompilerParams(vmem_limit_bytes=mib * 1024 * 1024)


def pack_kernel(here_ref, assignment_ref, given_ref, flat, points_ref, rows_ref, at_ref, sems):
    rows, width = points_ref.shape
    piece = rows // PIECES
    copies = [
        pltpu.make_async_copy(
            given_ref.at[pl.ds(k * piece, piece)], points_ref.at[pl.ds(k * piece, piece)], sems.at[k]
        )
        for k in range(PIECES)
    ]
    for copy in copies:
        copy.start()

    blocks = width // LANES // HALVES
    stride = blocks * SLOTS + TAIL
    earlier = lax.broadcasted_iota(jnp.int32, (LANES, LANES), 0)
    lane = lax.broadcasted_iota(jnp.int32, (LANES, LANES), 1)
    earlier = (earlier < lane).astype(jnp.float32).astype(jnp.bfloat16)
    line = lax.broadcasted_iota(jnp.int32, (OWNERS, LANES), 0)
    place = lax.broadcasted_iota(jnp.int32, (LANES, LANES), 0)
    seen = jnp.zeros((OWNERS, 1), jnp.float32)
    tags = jnp.zeros((OWNERS, LANES), jnp.float32)
    for i in range(rows // LANES):
        assigned = assignment_ref[i : i + 1, :]
        owner = assigned >> 8
        label = (assigned & (CL_OWN - 1)) + 1
        group = (owner >> 4) * 4 + (owner & 3)
        member = (owner >> 2) & 3
        hot = (line == group * SIDE + member).astype(jnp.float32)
        before = jnp.dot(
            hot.astype(jnp.bfloat16), earlier, preferred_element_type=jnp.float32
        )
        position = jnp.sum(hot * (before + seen), axis=0, keepdims=True).astype(jnp.int32)
        seen = seen + jnp.sum(hot, axis=1, keepdims=True)
        rows_ref[i : i + 1, :] = group * (HALVES * stride) + member * CAP + position
        at = (place == position + (here_ref[0] >> 7) * CAP).astype(jnp.float32)
        tags = tags + lax.dot_general(
            (hot * label.astype(jnp.float32)).astype(jnp.bfloat16),
            at.astype(jnp.bfloat16),
            (((1,), (1,)), ((), ())),
            preferred_element_type=jnp.float32,
        )
    listing = pltpu.make_async_copy(rows_ref, at_ref, sems.at[PIECES])
    listing.start()

    for g in range(MERGE):
        low = (g + 1) * stride - TAIL
        owners = g // HALVES * SIDE
        flat[low : low + SIDE, :] = tags[owners : owners + SIDE]
        flat[low + SIDE : low + TAIL, :] = jnp.zeros((TAIL - SIDE, LANES), jnp.float32)

    def clear(g, carry):
        start = pl.multiple_of(g * stride, 8)
        flat[pl.ds(start, stride - TAIL), :] = jnp.zeros((stride - TAIL, LANES), jnp.float32)
        return carry

    lax.fori_loop(0, MERGE, clear, 0)
    listing.wait()

    def put(i, carry):
        start = pl.multiple_of(i * LANES, LANES)
        for first in range(0, LANES, 8):
            ats = [at_ref[i, first + r] for r in range(8)]
            tiles = [
                points_ref[pl.ds(start + first, 8), k * LANES : (k + 1) * LANES]
                for k in range(HALVES * blocks)
            ]
            for r in range(8):
                for k, tile in enumerate(tiles):
                    at = ats[r] + (k // blocks * stride + k % blocks * SLOTS)
                    flat[pl.ds(at, 1), :] = tile[r : r + 1]
        return carry

    lines = piece // LANES
    for k, copy in enumerate(copies):
        copy.wait()
        lax.fori_loop(k * lines, (k + 1) * lines, put, 0)


def pack(here, assignment, points):
    rows, width = points.shape
    stride = width // LANES // HALVES * SLOTS + TAIL
    lines = (rows // LANES, LANES)
    packed = pl.pallas_call(
        pack_kernel,
        out_shape=jax.ShapeDtypeStruct((MERGE * stride, LANES), jnp.float32),
        in_specs=[whole(pltpu.SMEM), whole(), whole(pltpu.HBM)],
        out_specs=whole(),
        scratch_shapes=[
            pltpu.VMEM(points.shape, jnp.float32),
            pltpu.VMEM(lines, jnp.int32),
            pltpu.SMEM(lines, jnp.int32),
            pltpu.SemaphoreType.DMA((PIECES + 1,)),
        ],
        compiler_params=params(PACK_MIB),
        name="pack",
    )(here, assignment.reshape(lines), pltpu.with_memory_space_constraint(points, pltpu.HBM))
    return packed.reshape(MERGE, stride, LANES)


def merge_kernel(arrived_ref, out_ref, hot_ref, square_ref):
    blocks = (arrived_ref.shape[1] - TAIL) // SLOTS
    tail = blocks * SLOTS
    gather = LANES // CAP
    tiles = []
    for k in range(MERGE // gather):
        tile = arrived_ref[k * gather, tail:, :]
        for s in range(1, gather):
            tile = tile + arrived_ref[k * gather + s, tail:, :]
        tiles.append(tile)
    tags = jnp.concatenate(tiles, axis=1).astype(jnp.bfloat16)
    cluster = lax.broadcasted_iota(jnp.int32, (CL_OWN, KEYS), 0) + 1
    cluster = cluster.astype(jnp.float32).astype(jnp.bfloat16)
    one = jnp.ones((CL_OWN, KEYS), jnp.bfloat16)
    none = jnp.zeros((CL_OWN, KEYS), jnp.bfloat16)
    for m in range(SIDE):
        hot = jnp.where(cluster == tags[m : m + 1], one, none)
        hot_ref[m] = hot
        for j in range(blocks):
            low = j * SLOTS + m * CAP
            data = arrived_ref[:, low : low + CAP, :].reshape(KEYS, LANES)
            squares = data * data
            square_ref[...] = squares if j == 0 else square_ref[...] + squares
            terms = jnp.concatenate(split3(data)[:2], axis=1)
            total = jnp.dot(hot_ref[m], terms, preferred_element_type=jnp.float32)
            total = total[:, LANES:] + total[:, :LANES]
            for zp in range(SIDE):
                out_ref[m * SIDE + zp, j * ROWS : (j + 1) * ROWS, :] = total[
                    zp * ROWS : (zp + 1) * ROWS
                ]
        ones = jnp.ones((TAIL, LANES), jnp.bfloat16)
        norms = sum(
            lax.dot_general(
                ones, term, (((1,), (1,)), ((), ())), preferred_element_type=jnp.float32
            )
            for term in reversed(split3(square_ref[...]))
        )
        row = lax.broadcasted_iota(jnp.int32, (TAIL, KEYS), 0)
        values = jnp.where(row == 0, 1.0, 0.0)
        for k, term in enumerate(split3(norms), 1):
            values = jnp.where(row == k, term.astype(jnp.float32), values)
        small = lax.dot_general(
            values.astype(jnp.bfloat16),
            hot_ref[m],
            (((1,), (1,)), ((), ())),
            preferred_element_type=jnp.float32,
        )
        for zp in range(SIDE):
            low = zp * ROWS // LANES * LANES
            out_ref[m * SIDE + zp, blocks * ROWS :, :] = small[:, low : low + LANES]


def merge(arrived):
    blocks = (arrived.shape[1] - TAIL) // SLOTS
    return pl.pallas_call(
        merge_kernel,
        out_shape=jax.ShapeDtypeStruct((SIDE * SIDE, blocks * ROWS + TAIL, LANES), jnp.float32),
        in_specs=[whole()],
        out_specs=whole(),
        scratch_shapes=[
            pltpu.VMEM((SIDE, CL_OWN, KEYS), jnp.bfloat16),
            pltpu.VMEM((KEYS, LANES), jnp.float32),
        ],
        compiler_params=params(16),
        name="merge",
    )(arrived)


def finish_kernel(here_ref, arrived_ref, out_ref):
    total = arrived_ref[0]
    for k in range(1, SIDE * SIDE):
        total = total + arrived_ref[k]
    tail = total.shape[0] - TAIL
    row = lax.broadcasted_iota(jnp.int32, (ROWS, LANES), 0)
    lane = lax.broadcasted_iota(jnp.int32, (ROWS, LANES), 1)
    mine = lane == row + (here_ref[0] & (LANES - 1))
    counts = jnp.sum(jnp.where(mine, total[tail : tail + 1], 0.0), axis=1, keepdims=True)
    denom = jnp.maximum(counts, 1.0)
    norm = jnp.zeros((ROWS, LANES), jnp.float32)
    for low in range(0, tail, ROWS):
        sums = total[low : low + ROWS]
        norm = norm + sums * sums
        means = sums / denom
        for k in range(SIDE * HALVES):
            out_ref[k, low : low + ROWS, :] = means
    norm = jnp.sum(norm, axis=1, keepdims=True)
    norm = jnp.sum(jnp.where(mine, norm, 0.0), axis=0, keepdims=True)
    squares = total[tail + 1 : tail + 2] + total[tail + 2 : tail + 3] + total[tail + 3 : tail + 4]
    line = lax.broadcasted_iota(jnp.int32, (TAIL, LANES), 0)
    last = jnp.where(line == 0, total[tail : tail + 1], 0.0)
    last = jnp.where(line == 1, squares, last)
    last = jnp.where(line == 2, norm, last)
    for k in range(SIDE * HALVES):
        out_ref[k, tail:, :] = last


def finish(here, arrived):
    return pl.pallas_call(
        finish_kernel,
        out_shape=jax.ShapeDtypeStruct((SIDE * HALVES, *arrived.shape[1:]), jnp.float32),
        in_specs=[whole(pltpu.SMEM), whole()],
        out_specs=whole(),
        compiler_params=params(6),
        name="finish",
    )(here, arrived)


def lay_kernel(all_ref, centre_ref, spread_ref):
    width = centre_ref.shape[1]
    blocks = width // LANES // HALVES
    tail = blocks * ROWS
    for zp in range(SIDE):
        for zb in range(HALVES):
            for j in range(blocks):
                low = (zb * blocks + j) * LANES
                centre_ref[zp * ROWS : (zp + 1) * ROWS, low : low + LANES] = all_ref[
                    zp * HALVES + zb, j * ROWS : (j + 1) * ROWS, :
                ]
    share = LANES // ROWS
    for t in range(SIDE // share):
        first = t * share * HALVES
        denom = jnp.maximum(all_ref[first, tail : tail + 1, :], 1.0)
        squares = sum(all_ref[first + zb, tail + 1 : tail + 2, :] for zb in range(HALVES))
        norm = sum(all_ref[first + k, tail + 2 : tail + 3, :] for k in range(share * HALVES))
        spread_ref[t : t + 1, :] = (squares - norm / denom) / (denom * width)


def lay(gathered, width):
    return pl.pallas_call(
        lay_kernel,
        out_shape=[
            jax.ShapeDtypeStruct((CL_OWN, width), jnp.float32),
            jax.ShapeDtypeStruct((CL_OWN // LANES, LANES), jnp.float32),
        ],
        in_specs=[whole()],
        out_specs=[whole(), whole()],
        compiler_params=params(6),
        name="lay",
    )(gathered)


def body(points, assignment):
    width = points.shape[1]
    group = (lax.axis_index("c") * HALVES + lax.axis_index("zb")) % (LANES // CAP)
    offset = lax.axis_index("zp") * ROWS % LANES
    here = (group * LANES + offset).reshape(1)
    packed = pack(here, assignment, points)
    met = lax.all_to_all(packed, ("x", "yb", "c", "zb"), split_axis=0, concat_axis=0, tiled=True)
    partial = merge(met)
    partial = lax.all_to_all(partial, ("yp", "zp"), split_axis=0, concat_axis=0, tiled=True)
    done = finish(here, partial)
    gathered = lax.all_to_all(done, ("zp", "zb"), split_axis=0, concat_axis=0, tiled=True)
    centre, spread = lay(gathered, width)
    return centre, spread.reshape(CL_OWN)


def solution(mesh):
    fine = Mesh(mesh.devices.reshape(4, 2, 4, 4, 2, 2), ("zp", "zb", "x", "yp", "yb", "c"))
    every = ("zp", "zb", "x", "yp", "yb", "c")
    owners = ("x", "yp", "yb", "c")
    return jax.shard_map(
        body,
        mesh=fine,
        in_specs=(P(every, None), P(every)),
        out_specs=(P(owners, None), P(owners)),
        check_vma=False,
    )
```

```python
import jax
import jax.numpy as jnp
from jax import lax
from jax.experimental import pallas as pl
from jax.experimental.pallas import tpu as pltpu
from jax.sharding import Mesh
from jax.sharding import PartitionSpec as P

CL_OWN = 256
OWNERS = 64
LANES = 128
CAP = 32
SIDE = 4
GROUPS = OWNERS // SIDE
HALVES = 2
MERGE = GROUPS * HALVES
SLOTS = SIDE * CAP
ROWS = CL_OWN // SIDE
KEYS = MERGE * CAP
TAIL = 8
PIECES = 2
PACK_MIB = 12


def split3(value):
    first = value.astype(jnp.bfloat16)
    rest = value - first.astype(jnp.float32)
    second = rest.astype(jnp.bfloat16)
    third = (rest - second.astype(jnp.float32)).astype(jnp.bfloat16)
    return first, second, third


def whole(space=pltpu.VMEM):
    return pl.BlockSpec(memory_space=space)


def params(mib):
    return pltpu.CompilerParams(vmem_limit_bytes=mib * 1024 * 1024)


def pack_kernel(
    here_ref, labels_ref, given_ref, flat, points_ref, assignment_ref, rows_ref, at_ref, sems
):
    rows, width = points_ref.shape
    piece = rows // PIECES
    fetch = pltpu.make_async_copy(labels_ref, assignment_ref, sems.at[PIECES + 1])
    fetch.start()
    copies = [
        pltpu.make_async_copy(
            given_ref.at[pl.ds(k * piece, piece)], points_ref.at[pl.ds(k * piece, piece)], sems.at[k]
        )
        for k in range(PIECES)
    ]
    for copy in copies:
        copy.start()

    blocks = width // LANES // HALVES
    stride = blocks * SLOTS + TAIL

    def clear(g, carry):
        start = pl.multiple_of(g * stride, 8)
        flat[pl.ds(start, stride - TAIL), :] = jnp.zeros((stride - TAIL, LANES), jnp.float32)
        return carry

    lax.fori_loop(0, MERGE // 2, clear, 0)
    fetch.wait()
    earlier = lax.broadcasted_iota(jnp.int32, (LANES, LANES), 0)
    lane = lax.broadcasted_iota(jnp.int32, (LANES, LANES), 1)
    earlier = (earlier < lane).astype(jnp.float32).astype(jnp.bfloat16)
    line = lax.broadcasted_iota(jnp.int32, (OWNERS, LANES), 0)
    place = lax.broadcasted_iota(jnp.int32, (LANES, LANES), 0)
    seen = jnp.zeros((OWNERS, 1), jnp.float32)
    tags = jnp.zeros((OWNERS, LANES), jnp.float32)
    for i in range(rows // LANES):
        assigned = assignment_ref[i : i + 1, :]
        owner = assigned >> 8
        label = (assigned & (CL_OWN - 1)) + 1
        group = (owner >> 4) * 4 + (owner & 3)
        member = (owner >> 2) & 3
        hot = (line == group * SIDE + member).astype(jnp.float32)
        before = jnp.dot(
            hot.astype(jnp.bfloat16), earlier, preferred_element_type=jnp.float32
        )
        position = jnp.sum(hot * (before + seen), axis=0, keepdims=True).astype(jnp.int32)
        seen = seen + jnp.sum(hot, axis=1, keepdims=True)
        rows_ref[i : i + 1, :] = group * stride + member * CAP + position
        at = (place == position + (here_ref[0] >> 7) * CAP).astype(jnp.float32)
        tags = tags + lax.dot_general(
            (hot * label.astype(jnp.float32)).astype(jnp.bfloat16),
            at.astype(jnp.bfloat16),
            (((1,), (1,)), ((), ())),
            preferred_element_type=jnp.float32,
        )
    listing = pltpu.make_async_copy(rows_ref, at_ref, sems.at[PIECES])
    listing.start()

    for g in range(MERGE):
        low = (g + 1) * stride - TAIL
        owners = (g % GROUPS) * SIDE
        flat[low : low + SIDE, :] = tags[owners : owners + SIDE]
        flat[low + SIDE : low + TAIL, :] = jnp.zeros((TAIL - SIDE, LANES), jnp.float32)

    lax.fori_loop(MERGE // 2, MERGE, clear, 0)
    listing.wait()

    def put(i, carry):
        start = pl.multiple_of(i * LANES, LANES)
        for first in range(0, LANES, 8):
            ats = [at_ref[i, first + r] for r in range(8)]
            tiles = [
                points_ref[pl.ds(start + first, 8), k * LANES : (k + 1) * LANES]
                for k in range(HALVES * blocks)
            ]
            for r in range(8):
                for k, tile in enumerate(tiles):
                    at = ats[r] + (k // blocks * GROUPS * stride + k % blocks * SLOTS)
                    flat[pl.ds(at, 1), :] = tile[r : r + 1]
        return carry

    lines = piece // LANES
    for k, copy in enumerate(copies):
        copy.wait()
        lax.fori_loop(k * lines, (k + 1) * lines, put, 0)


def pack(here, assignment, points):
    rows, width = points.shape
    stride = width // LANES // HALVES * SLOTS + TAIL
    lines = (rows // LANES, LANES)
    packed = pl.pallas_call(
        pack_kernel,
        out_shape=jax.ShapeDtypeStruct((MERGE * stride, LANES), jnp.float32),
        in_specs=[whole(pltpu.SMEM), whole(pltpu.HBM), whole(pltpu.HBM)],
        out_specs=whole(),
        scratch_shapes=[
            pltpu.VMEM(points.shape, jnp.float32),
            pltpu.VMEM(lines, jnp.int32),
            pltpu.VMEM(lines, jnp.int32),
            pltpu.SMEM(lines, jnp.int32),
            pltpu.SemaphoreType.DMA((PIECES + 2,)),
        ],
        compiler_params=params(PACK_MIB),
        name="pack",
    )(here, pltpu.with_memory_space_constraint(assignment.reshape(lines), pltpu.HBM), pltpu.with_memory_space_constraint(points, pltpu.HBM))
    return packed.reshape(MERGE, stride, LANES)


def merge_kernel(arrived_ref, out_ref, hot_ref, square_ref):
    blocks = (arrived_ref.shape[1] - TAIL) // SLOTS
    tail = blocks * SLOTS
    gather = LANES // CAP
    tiles = []
    for k in range(MERGE // gather):
        tile = arrived_ref[k * gather, tail:, :]
        for s in range(1, gather):
            tile = tile + arrived_ref[k * gather + s, tail:, :]
        tiles.append(tile)
    tags = jnp.concatenate(tiles, axis=1).astype(jnp.bfloat16)
    cluster = lax.broadcasted_iota(jnp.int32, (CL_OWN, KEYS), 0) + 1
    cluster = cluster.astype(jnp.float32).astype(jnp.bfloat16)
    one = jnp.ones((CL_OWN, KEYS), jnp.bfloat16)
    none = jnp.zeros((CL_OWN, KEYS), jnp.bfloat16)
    for m in range(SIDE):
        hot = jnp.where(cluster == tags[m : m + 1], one, none)
        hot_ref[m] = hot
        for j in range(blocks):
            low = j * SLOTS + m * CAP
            data = arrived_ref[:, low : low + CAP, :].reshape(KEYS, LANES)
            squares = data * data
            square_ref[...] = squares if j == 0 else square_ref[...] + squares
            terms = jnp.concatenate(split3(data)[:2], axis=1)
            total = jnp.dot(hot_ref[m], terms, preferred_element_type=jnp.float32)
            total = total[:, LANES:] + total[:, :LANES]
            for zp in range(SIDE):
                out_ref[m * SIDE + zp, j * ROWS : (j + 1) * ROWS, :] = total[
                    zp * ROWS : (zp + 1) * ROWS
                ]
        ones = jnp.ones((TAIL, LANES), jnp.bfloat16)
        norms = sum(
            lax.dot_general(
                ones, term, (((1,), (1,)), ((), ())), preferred_element_type=jnp.float32
            )
            for term in reversed(split3(square_ref[...]))
        )
        row = lax.broadcasted_iota(jnp.int32, (TAIL, KEYS), 0)
        values = jnp.where(row == 0, 1.0, 0.0)
        for k, term in enumerate(split3(norms), 1):
            values = jnp.where(row == k, term.astype(jnp.float32), values)
        small = lax.dot_general(
            values.astype(jnp.bfloat16),
            hot_ref[m],
            (((1,), (1,)), ((), ())),
            preferred_element_type=jnp.float32,
        )
        for zp in range(SIDE):
            low = zp * ROWS // LANES * LANES
            out_ref[m * SIDE + zp, blocks * ROWS :, :] = small[:, low : low + LANES]


def merge(arrived):
    blocks = (arrived.shape[1] - TAIL) // SLOTS
    return pl.pallas_call(
        merge_kernel,
        out_shape=jax.ShapeDtypeStruct((SIDE * SIDE, blocks * ROWS + TAIL, LANES), jnp.float32),
        in_specs=[whole()],
        out_specs=whole(),
        scratch_shapes=[
            pltpu.VMEM((SIDE, CL_OWN, KEYS), jnp.bfloat16),
            pltpu.VMEM((KEYS, LANES), jnp.float32),
        ],
        compiler_params=params(16),
        name="merge",
    )(arrived)


def finish_kernel(here_ref, arrived_ref, out_ref):
    total = arrived_ref[0]
    for k in range(1, SIDE * SIDE):
        total = total + arrived_ref[k]
    tail = total.shape[0] - TAIL
    row = lax.broadcasted_iota(jnp.int32, (ROWS, LANES), 0)
    lane = lax.broadcasted_iota(jnp.int32, (ROWS, LANES), 1)
    mine = lane == row + (here_ref[0] & (LANES - 1))
    counts = jnp.sum(jnp.where(mine, total[tail : tail + 1], 0.0), axis=1, keepdims=True)
    denom = jnp.maximum(counts, 1.0)
    norm = jnp.zeros((ROWS, LANES), jnp.float32)
    for low in range(0, tail, ROWS):
        sums = total[low : low + ROWS]
        norm = norm + sums * sums
        means = sums / denom
        for k in range(SIDE * HALVES):
            out_ref[k, low : low + ROWS, :] = means
    norm = jnp.sum(norm, axis=1, keepdims=True)
    norm = jnp.sum(jnp.where(mine, norm, 0.0), axis=0, keepdims=True)
    squares = total[tail + 1 : tail + 2] + total[tail + 2 : tail + 3] + total[tail + 3 : tail + 4]
    line = lax.broadcasted_iota(jnp.int32, (TAIL, LANES), 0)
    last = jnp.where(line == 0, total[tail : tail + 1], 0.0)
    last = jnp.where(line == 1, squares, last)
    last = jnp.where(line == 2, norm, last)
    for k in range(SIDE * HALVES):
        out_ref[k, tail:, :] = last


def finish(here, arrived):
    return pl.pallas_call(
        finish_kernel,
        out_shape=jax.ShapeDtypeStruct((SIDE * HALVES, *arrived.shape[1:]), jnp.float32),
        in_specs=[whole(pltpu.SMEM), whole()],
        out_specs=whole(),
        compiler_params=params(6),
        name="finish",
    )(here, arrived)


def lay_kernel(all_ref, centre_ref, spread_ref):
    width = centre_ref.shape[1]
    blocks = width // LANES // HALVES
    tail = blocks * ROWS
    for zp in range(SIDE):
        for zb in range(HALVES):
            for j in range(blocks):
                low = (zb * blocks + j) * LANES
                centre_ref[zp * ROWS : (zp + 1) * ROWS, low : low + LANES] = all_ref[
                    zp * HALVES + zb, j * ROWS : (j + 1) * ROWS, :
                ]
    share = LANES // ROWS
    for t in range(SIDE // share):
        first = t * share * HALVES
        denom = jnp.maximum(all_ref[first, tail : tail + 1, :], 1.0)
        squares = sum(all_ref[first + zb, tail + 1 : tail + 2, :] for zb in range(HALVES))
        norm = sum(all_ref[first + k, tail + 2 : tail + 3, :] for k in range(share * HALVES))
        spread_ref[t : t + 1, :] = (squares - norm / denom) / (denom * width)


def lay(gathered, width):
    return pl.pallas_call(
        lay_kernel,
        out_shape=[
            jax.ShapeDtypeStruct((CL_OWN, width), jnp.float32),
            jax.ShapeDtypeStruct((CL_OWN // LANES, LANES), jnp.float32),
        ],
        in_specs=[whole()],
        out_specs=[whole(), whole()],
        compiler_params=params(6),
        name="lay",
    )(gathered)


def body(points, assignment):
    width = points.shape[1]
    group = (lax.axis_index("yb") * 2 + lax.axis_index("c")) % (LANES // CAP)
    offset = lax.axis_index("zp") * ROWS % LANES
    here = (group * LANES + offset).reshape(1)
    packed = pack(here, assignment, points)
    met = lax.all_to_all(packed, ("zb", "x", "yb", "c"), split_axis=0, concat_axis=0, tiled=True)
    partial = merge(met)
    partial = lax.all_to_all(partial, ("yp", "zp"), split_axis=0, concat_axis=0, tiled=True)
    done = finish(here, partial)
    gathered = lax.all_to_all(done, ("zp", "zb"), split_axis=0, concat_axis=0, tiled=True)
    centre, spread = lay(gathered, width)
    return centre, spread.reshape(CL_OWN)


def solution(mesh):
    fine = Mesh(mesh.devices.reshape(4, 2, 4, 4, 2, 2), ("zp", "zb", "x", "yp", "yb", "c"))
    every = ("zp", "zb", "x", "yp", "yb", "c")
    owners = ("x", "yp", "yb", "c")
    return jax.shard_map(
        body,
        mesh=fine,
        in_specs=(P(every, None), P(every)),
        out_specs=(P(owners, None), P(owners)),
        check_vma=False,
    )
```

```python
import jax
import jax.numpy as jnp
from jax import lax
from jax.experimental import pallas as pl
from jax.experimental.pallas import tpu as pltpu
from jax.sharding import Mesh
from jax.sharding import PartitionSpec as P

CL_OWN = 256
OWNERS = 64
LANES = 128
CAP = 32
SIDE = 4
GROUPS = OWNERS // SIDE
HALVES = 2
MERGE = GROUPS * HALVES
SLOTS = SIDE * CAP
ROWS = CL_OWN // SIDE
KEYS = MERGE * CAP
TAIL = 8
PIECES = 2
PACK_MIB = 12


def split3(value):
    first = value.astype(jnp.bfloat16)
    rest = value - first.astype(jnp.float32)
    second = rest.astype(jnp.bfloat16)
    third = (rest - second.astype(jnp.float32)).astype(jnp.bfloat16)
    return first, second, third


def whole(space=pltpu.VMEM):
    return pl.BlockSpec(memory_space=space)


def params(mib):
    return pltpu.CompilerParams(vmem_limit_bytes=mib * 1024 * 1024)


def pack_kernel(
    here_ref, labels_ref, given_ref, flat, points_ref, assignment_ref, rows_ref, at_ref, sems
):
    rows, width = points_ref.shape
    piece = rows // PIECES
    fetch = pltpu.make_async_copy(labels_ref, assignment_ref, sems.at[PIECES + 1])
    fetch.start()
    copies = [
        pltpu.make_async_copy(
            given_ref.at[pl.ds(k * piece, piece)], points_ref.at[pl.ds(k * piece, piece)], sems.at[k]
        )
        for k in range(PIECES)
    ]
    for copy in copies:
        copy.start()

    blocks = width // LANES // HALVES
    stride = blocks * SLOTS + TAIL

    def clear(g, carry):
        start = pl.multiple_of(g * stride, 8)
        flat[pl.ds(start, stride - TAIL), :] = jnp.zeros((stride - TAIL, LANES), jnp.float32)
        return carry

    lax.fori_loop(0, MERGE // 2, clear, 0)
    fetch.wait()
    earlier = lax.broadcasted_iota(jnp.int32, (LANES, LANES), 0)
    lane = lax.broadcasted_iota(jnp.int32, (LANES, LANES), 1)
    earlier = (earlier < lane).astype(jnp.float32).astype(jnp.bfloat16)
    line = lax.broadcasted_iota(jnp.int32, (OWNERS, LANES), 0)
    place = lax.broadcasted_iota(jnp.int32, (LANES, LANES), 0)
    seen = jnp.zeros((OWNERS, 1), jnp.float32)
    tags = jnp.zeros((OWNERS, LANES), jnp.float32)
    for i in range(rows // LANES):
        assigned = assignment_ref[i : i + 1, :]
        owner = assigned >> 8
        label = (assigned & (CL_OWN - 1)) + 1
        group = (owner >> 4) * 4 + (owner & 3)
        member = (owner >> 2) & 3
        hot = (line == group * SIDE + member).astype(jnp.float32)
        before = jnp.dot(
            hot.astype(jnp.bfloat16), earlier, preferred_element_type=jnp.float32
        )
        position = jnp.sum(hot * (before + seen), axis=0, keepdims=True).astype(jnp.int32)
        seen = seen + jnp.sum(hot, axis=1, keepdims=True)
        rows_ref[i : i + 1, :] = group * stride + member * CAP + position
        at = (place == position + (here_ref[0] >> 7) * CAP).astype(jnp.float32)
        tags = tags + lax.dot_general(
            (hot * label.astype(jnp.float32)).astype(jnp.bfloat16),
            at.astype(jnp.bfloat16),
            (((1,), (1,)), ((), ())),
            preferred_element_type=jnp.float32,
        )
    listing = pltpu.make_async_copy(rows_ref, at_ref, sems.at[PIECES])
    listing.start()

    for g in range(MERGE):
        low = (g + 1) * stride - TAIL
        owners = (g % GROUPS) * SIDE
        flat[low : low + SIDE, :] = tags[owners : owners + SIDE]
        flat[low + SIDE : low + TAIL, :] = jnp.zeros((TAIL - SIDE, LANES), jnp.float32)

    lax.fori_loop(MERGE // 2, MERGE, clear, 0)
    listing.wait()

    def put(i, carry):
        start = pl.multiple_of(i * LANES, LANES)
        for first in range(0, LANES, 8):
            ats = [at_ref[i, first + r] for r in range(8)]
            tiles = [
                points_ref[pl.ds(start + first, 8), k * LANES : (k + 1) * LANES]
                for k in range(HALVES * blocks)
            ]
            for r in range(8):
                for k, tile in enumerate(tiles):
                    at = ats[r] + (k // blocks * GROUPS * stride + k % blocks * SLOTS)
                    flat[pl.ds(at, 1), :] = tile[r : r + 1]
        return carry

    lines = piece // LANES
    for k, copy in enumerate(copies):
        copy.wait()
        lax.fori_loop(k * lines, (k + 1) * lines, put, 0)


def pack(here, assignment, points):
    rows, width = points.shape
    stride = width // LANES // HALVES * SLOTS + TAIL
    lines = (rows // LANES, LANES)
    packed = pl.pallas_call(
        pack_kernel,
        out_shape=jax.ShapeDtypeStruct((MERGE * stride, LANES), jnp.float32),
        in_specs=[whole(pltpu.SMEM), whole(pltpu.HBM), whole(pltpu.HBM)],
        out_specs=whole(),
        scratch_shapes=[
            pltpu.VMEM(points.shape, jnp.float32),
            pltpu.VMEM(lines, jnp.int32),
            pltpu.VMEM(lines, jnp.int32),
            pltpu.SMEM(lines, jnp.int32),
            pltpu.SemaphoreType.DMA((PIECES + 2,)),
        ],
        compiler_params=params(PACK_MIB),
        name="pack",
    )(here, pltpu.with_memory_space_constraint(assignment.reshape(lines), pltpu.HBM), pltpu.with_memory_space_constraint(points, pltpu.HBM))
    return packed.reshape(MERGE, stride, LANES)


def merge_kernel(arrived_ref, out_ref, hot_ref, square_ref):
    blocks = (arrived_ref.shape[1] - TAIL) // SLOTS
    tail = blocks * SLOTS
    gather = LANES // CAP
    tiles = []
    for k in range(MERGE // gather):
        tile = arrived_ref[k * gather, tail:, :]
        for s in range(1, gather):
            tile = tile + arrived_ref[k * gather + s, tail:, :]
        tiles.append(tile)
    tags = jnp.concatenate(tiles, axis=1).astype(jnp.bfloat16)
    cluster = lax.broadcasted_iota(jnp.int32, (CL_OWN, KEYS), 0) + 1
    cluster = cluster.astype(jnp.float32).astype(jnp.bfloat16)
    one = jnp.ones((CL_OWN, KEYS), jnp.bfloat16)
    none = jnp.zeros((CL_OWN, KEYS), jnp.bfloat16)
    for m in range(SIDE):
        hot = jnp.where(cluster == tags[m : m + 1], one, none)
        hot_ref[m] = hot
        for j in range(blocks):
            low = j * SLOTS + m * CAP
            data = arrived_ref[:, low : low + CAP, :].reshape(KEYS, LANES)
            squares = data * data
            square_ref[...] = squares if j == 0 else square_ref[...] + squares
            terms = jnp.concatenate(split3(data)[:2], axis=1)
            total = jnp.dot(hot_ref[m], terms, preferred_element_type=jnp.float32)
            total = total[:, LANES:] + total[:, :LANES]
            for zp in range(SIDE):
                out_ref[m * SIDE + zp, j * ROWS : (j + 1) * ROWS, :] = total[
                    zp * ROWS : (zp + 1) * ROWS
                ]
        ones = jnp.ones((TAIL, LANES), jnp.bfloat16)
        norms = sum(
            lax.dot_general(
                ones, term, (((1,), (1,)), ((), ())), preferred_element_type=jnp.float32
            )
            for term in reversed(split3(square_ref[...]))
        )
        row = lax.broadcasted_iota(jnp.int32, (TAIL, KEYS), 0)
        values = jnp.where(row == 0, 1.0, 0.0)
        for k, term in enumerate(split3(norms), 1):
            values = jnp.where(row == k, term.astype(jnp.float32), values)
        small = lax.dot_general(
            values.astype(jnp.bfloat16),
            hot_ref[m],
            (((1,), (1,)), ((), ())),
            preferred_element_type=jnp.float32,
        )
        for zp in range(SIDE):
            low = zp * ROWS // LANES * LANES
            out_ref[m * SIDE + zp, blocks * ROWS :, :] = small[:, low : low + LANES]


def merge(arrived):
    blocks = (arrived.shape[1] - TAIL) // SLOTS
    return pl.pallas_call(
        merge_kernel,
        out_shape=jax.ShapeDtypeStruct((SIDE * SIDE, blocks * ROWS + TAIL, LANES), jnp.float32),
        in_specs=[whole()],
        out_specs=whole(),
        scratch_shapes=[
            pltpu.VMEM((SIDE, CL_OWN, KEYS), jnp.bfloat16),
            pltpu.VMEM((KEYS, LANES), jnp.float32),
        ],
        compiler_params=params(16),
        name="merge",
    )(arrived)


def finish_kernel(here_ref, arrived_ref, out_ref):
    total = arrived_ref[0]
    for k in range(1, SIDE * SIDE):
        total = total + arrived_ref[k]
    tail = total.shape[0] - TAIL
    row = lax.broadcasted_iota(jnp.int32, (ROWS, LANES), 0)
    lane = lax.broadcasted_iota(jnp.int32, (ROWS, LANES), 1)
    mine = lane == row + (here_ref[0] & (LANES - 1))
    counts = jnp.sum(jnp.where(mine, total[tail : tail + 1], 0.0), axis=1, keepdims=True)
    denom = jnp.maximum(counts, 1.0)
    norm = jnp.zeros((ROWS, LANES), jnp.float32)
    for low in range(0, tail, ROWS):
        sums = total[low : low + ROWS]
        norm = norm + sums * sums
        out_ref[low : low + ROWS, :] = sums / denom
    norm = jnp.sum(norm, axis=1, keepdims=True)
    norm = jnp.sum(jnp.where(mine, norm, 0.0), axis=0, keepdims=True)
    squares = total[tail + 1 : tail + 2] + total[tail + 2 : tail + 3] + total[tail + 3 : tail + 4]
    line = lax.broadcasted_iota(jnp.int32, (TAIL, LANES), 0)
    last = jnp.where(line == 0, total[tail : tail + 1], 0.0)
    last = jnp.where(line == 1, squares, last)
    out_ref[tail:, :] = jnp.where(line == 2, norm, last)


def finish(here, arrived):
    return pl.pallas_call(
        finish_kernel,
        out_shape=jax.ShapeDtypeStruct(arrived.shape[1:], jnp.float32),
        in_specs=[whole(pltpu.SMEM), whole()],
        out_specs=whole(),
        compiler_params=params(6),
        name="finish",
    )(here, arrived)


def lay_kernel(all_ref, centre_ref, spread_ref):
    width = centre_ref.shape[1]
    blocks = width // LANES // HALVES
    tail = blocks * ROWS
    for zp in range(SIDE):
        for zb in range(HALVES):
            for j in range(blocks):
                low = (zb * blocks + j) * LANES
                centre_ref[zp * ROWS : (zp + 1) * ROWS, low : low + LANES] = all_ref[
                    zp * HALVES + zb, j * ROWS : (j + 1) * ROWS, :
                ]
    share = LANES // ROWS
    for t in range(SIDE // share):
        first = t * share * HALVES
        denom = jnp.maximum(all_ref[first, tail : tail + 1, :], 1.0)
        squares = sum(all_ref[first + zb, tail + 1 : tail + 2, :] for zb in range(HALVES))
        norm = sum(all_ref[first + k, tail + 2 : tail + 3, :] for k in range(share * HALVES))
        spread_ref[t : t + 1, :] = (squares - norm / denom) / (denom * width)


def lay(gathered, width):
    return pl.pallas_call(
        lay_kernel,
        out_shape=[
            jax.ShapeDtypeStruct((CL_OWN, width), jnp.float32),
            jax.ShapeDtypeStruct((CL_OWN // LANES, LANES), jnp.float32),
        ],
        in_specs=[whole()],
        out_specs=[whole(), whole()],
        compiler_params=params(6),
        name="lay",
    )(gathered)


def body(points, assignment):
    width = points.shape[1]
    group = (lax.axis_index("yb") * 2 + lax.axis_index("c")) % (LANES // CAP)
    offset = lax.axis_index("zp") * ROWS % LANES
    here = (group * LANES + offset).reshape(1)
    packed = pack(here, assignment, points)
    met = lax.all_to_all(packed, ("zb", "x", "yb", "c"), split_axis=0, concat_axis=0, tiled=True)
    partial = merge(met)
    partial = lax.all_to_all(partial, ("yp", "zp"), split_axis=0, concat_axis=0, tiled=True)
    done = finish(here, partial)
    gathered = lax.all_gather(done, ("zp", "zb"), axis=0, tiled=False)
    centre, spread = lay(gathered, width)
    return centre, spread.reshape(CL_OWN)


def solution(mesh):
    fine = Mesh(mesh.devices.reshape(4, 2, 4, 4, 2, 2), ("zp", "zb", "x", "yp", "yb", "c"))
    every = ("zp", "zb", "x", "yp", "yb", "c")
    owners = ("x", "yp", "yb", "c")
    return jax.shard_map(
        body,
        mesh=fine,
        in_specs=(P(every, None), P(every)),
        out_specs=(P(owners, None), P(owners)),
        check_vma=False,
    )
```
